256 devices in a mesh: ctx: 16 (over y_hi, z), tp: 8 (over x, y_lo), probe: 2 (over core).
Axes of the slice: x: 4, y: 4 (y_hi: 2, y_lo: 2; y = y_hi * 2 + y_lo), z: 8, core: 2. Of those that a mesh axis runs over, the one named last changes fastest.
Arguments:
- latent: float32 [2048, 3072], P('ctx', 'tp'), may hold values from -6 to 6
- probes: int32 [2, 2048, 3072], P('probe', 'ctx', 'tp'), may hold values from 0 to 1
- modulation: float32 [2, 3, 3072], replicated, may hold values from -3 to 3
- pattern: int32 [16, 8], P('ctx'), may hold values from 0 to 15, as said below
- w_qkv: bfloat16 [3072, 3, 3072], P(None, None, 'tp'), may hold values from -0.109375 to 0.109375
- w_out: bfloat16 [3072, 3072], P('tp'), may hold values from -0.109375 to 0.109375
- w_up: bfloat16 [3072, 6144], P('ctx', 'tp'), may hold values from -0.109375 to 0.109375
- w_down: bfloat16 [6144, 3072], P('tp', 'ctx'), may hold values from -0.078125 to 0.078125
- q_gain: float32 [3072], P('tp'), may hold values from 0.5 to 5.1, as said below
- k_gain: float32 [3072], P('tp'), may hold values from 0.5 to 2
Outputs:
- latent_out: float32 [2048, 3072], P('ctx', 'tp')
- density_change: float32 [2048], P('ctx')
The draws below stay inside these ranges and needn't reach their ends.
Inputs may be any that keep to these rules, and one draw needn't show every extreme that they name: `pattern`: row q lists key blocks for query block q: its first entry is q; the next entries are distinct blocks other than q up to a count of 1 to 8, after which every entry is q again; row 0 lists 8 distinct blocks. `q_gain`: positive gains.
All inputs are finite; a program needn't handle non-finite values.
Results may differ from the reference program's by a relative error of at most 0.034.
Values may be sent and summed in bfloat16 or wider, within the bound.
A program may use at most 128 MiB of HBM per device.

```python
import math
import jax
import jax.numpy as jnp
from jax import lax

D = 3072
H = 24
HD = 128
FF = 6144
BLK = 128
K_SEL = 8
STEPS = 2
TOKENS = 2048
NB = 16
PROBES = 2
N_TP = 8


def draw_pattern(key, part):
    blocks = jnp.arange(NB, dtype=jnp.int32)
    row_keys = jax.random.split(jax.random.fold_in(key, 11), NB)
    offsets = jax.vmap(lambda row_key: jax.random.permutation(row_key, NB - 1)[:K_SEL - 1])(row_keys) + 1
    counts = jax.random.randint(jax.random.fold_in(key, 12), (NB,), 1, K_SEL + 1)
    counts = counts.at[0].set(K_SEL)
    others = (blocks[:, None] + offsets.astype(jnp.int32)) % NB
    columns = jnp.arange(1, K_SEL, dtype=jnp.int32)
    others = jnp.where(columns[None, :] < counts[:, None], others, blocks[:, None])
    return jnp.concatenate([blocks[:, None], others], axis=1).astype(jnp.int32)


def draw_q_gain(key, part):
    head_level = jax.random.uniform(jax.random.fold_in(key, 21), (H, 1), jnp.float32)
    fine_level = jax.random.uniform(jax.random.fold_in(key, 22), (H, HD), jnp.float32, 0.8, 1.25)
    head_scale = jnp.exp((head_level - 0.5) * math.log(2.0))
    return (head_scale * fine_level).reshape(H * HD).astype(jnp.float32)


def plant(array, stream_key, low, high):
    dims = array.shape
    index_at = [jax.random.randint(jax.random.fold_in(stream_key, axis), (), 0, dims[axis]) for axis in range(len(dims))]
    array = array.at[tuple(index_at)].set(low)
    longest = dims.index(max(dims))
    index_at[longest] = (index_at[longest] + 1) % dims[longest]
    return array.at[tuple(index_at)].set(high)


def levels(own_key, extent, cuts, least, high):
    loudness = 1.0
    for position, blocks in cuts:
        heights = jax.random.uniform(jax.random.fold_in(jax.random.fold_in(own_key, 6), position), (blocks,), jnp.float32, least / len(cuts), high / len(cuts))
        loudness = loudness * jnp.repeat(jnp.exp(heights), extent[position] // blocks).reshape((-1,) + (1,) * (len(extent) - 1 - position))
    return loudness


def gaussian(stream_key, extent, scale, bound, pieces=(), kind=jnp.bfloat16):
    entries = scale * jax.random.normal(stream_key, extent, jnp.float32)
    if pieces:
        entries = entries * levels(stream_key, extent, pieces, -0.22, 0.18)
    return jnp.clip(entries, -bound, bound).astype(kind)


def setup_inputs(seed: int = 0) -> dict:
    keys = jax.random.split(jax.random.key(seed), 11)
    return {
        "latent": gaussian(keys[0], (TOKENS, D), 1.0, 6.0, ((0, 16), (1, 8)), jnp.float32),
        "probes": plant(jax.random.randint(keys[1], (PROBES, TOKENS, D), 0, 2), jax.random.fold_in(keys[1], 1), 0, 1).astype(jnp.int32),
        "modulation": gaussian(keys[2], (STEPS, 3, D), 0.5, 3.0, (), jnp.float32),
        "pattern": draw_pattern(jax.random.fold_in(keys[10], 71), 0),
        "w_qkv": gaussian(keys[4], (D, 3, H * HD), D ** -0.5, 0.109375, ((2, 8),)),
        "w_out": gaussian(keys[5], (H * HD, D), (H * HD) ** -0.5, 0.109375, ((0, 8),)),
        "w_up": gaussian(keys[6], (D, FF), D ** -0.5, 0.109375, ((0, 16), (1, 8))),
        "w_down": gaussian(keys[7], (FF, D), FF ** -0.5, 0.078125, ((0, 8), (1, 16))),
        "q_gain": draw_q_gain(jax.random.fold_in(keys[10], 71), 0),
        "k_gain": jnp.clip(jnp.exp(math.log(2.0) - 1.3862944 * jax.random.uniform(keys[9], (H * HD,), jnp.float32) ** levels(keys[9], (H * HD,), ((0, 8),), -0.2, 0.2)), 0.5, 2.0),
    }


EPS = 1e-06

def rounded(values):
    return lax.optimization_barrier(values.astype(jnp.bfloat16)).astype(jnp.float32)

def layer_norm(rows):
    row_mean = lax.optimization_barrier(jnp.mean(rows, axis=-1, keepdims=True))
    row_var = lax.optimization_barrier(jnp.mean(rows * rows, axis=-1, keepdims=True)) - row_mean * row_mean
    return (rows - row_mean) * lax.rsqrt(row_var + EPS)

def head_norm(projected, head_gain):
    head_view = projected.reshape(projected.shape[0], H, HD)
    inv_std = lax.rsqrt(lax.optimization_barrier(jnp.mean(head_view * head_view, axis=-1, keepdims=True)) + EPS)
    return (head_view * inv_std * head_gain.reshape(H, HD)).astype(jnp.bfloat16)

def block_mask(pattern):
    blocks = jnp.arange(NB, dtype=jnp.int32)
    listed = jnp.any(pattern[:, :, None] == blocks[None, None, :], axis=1)
    return jnp.repeat(jnp.repeat(listed, BLK, axis=0), BLK, axis=1)

def velocity(latent, mod_row, allowed, w_qkv, w_out, w_up, w_down, q_gain, k_gain):
    normed = (layer_norm(latent) * (1.0 + mod_row[1]) + mod_row[0]).astype(jnp.bfloat16)
    q_proj = jnp.dot(normed, w_qkv[:, 0], preferred_element_type=jnp.float32)
    k_proj = jnp.dot(normed, w_qkv[:, 1], preferred_element_type=jnp.float32)
    v_proj = jnp.dot(normed, w_qkv[:, 2], preferred_element_type=jnp.float32)
    q_rows = head_norm(q_proj, q_gain)
    k_rows = head_norm(k_proj, k_gain)
    v_rows = v_proj.astype(jnp.bfloat16).reshape(TOKENS, H, HD)

    def one_head(items):
        query_rows, key_rows, value_rows = items
        scores = jnp.dot(query_rows, key_rows.T, preferred_element_type=jnp.float32) / math.sqrt(HD)
        scores = jnp.where(allowed, scores, -1e+30)
        weights = jax.nn.softmax(scores, axis=-1)
        return jnp.dot(weights, value_rows.astype(jnp.float32), precision=lax.Precision.HIGHEST)
    outputs = lax.map(one_head, (q_rows.transpose(1, 0, 2), k_rows.transpose(1, 0, 2), v_rows.transpose(1, 0, 2)))
    attended = outputs.transpose(1, 0, 2).reshape(TOKENS, H * HD).astype(jnp.bfloat16)
    hidden = jax.nn.gelu(jnp.dot(normed, w_up, preferred_element_type=jnp.float32), approximate=True).astype(jnp.bfloat16)
    head_cols = H * HD // N_TP
    hidden_cols = FF // N_TP
    branch_sum = jnp.zeros((TOKENS, D), jnp.float32)
    for group in range(N_TP):
        group_part = jnp.dot(attended[:, group * head_cols:(group + 1) * head_cols], w_out[group * head_cols:(group + 1) * head_cols], preferred_element_type=jnp.float32)
        group_part = group_part + jnp.dot(hidden[:, group * hidden_cols:(group + 1) * hidden_cols], w_down[group * hidden_cols:(group + 1) * hidden_cols], preferred_element_type=jnp.float32)
        branch_sum = branch_sum + rounded(group_part)
    return mod_row[2] * branch_sum

def reference(latent, probes, modulation, pattern, w_qkv, w_out, w_up, w_down, q_gain, k_gain):
    allowed = block_mask(pattern)
    probe_signs = 2.0 * probes.astype(jnp.float32) - 1.0
    change = jnp.zeros((TOKENS,), jnp.float32)
    step_size = 1.0 / STEPS
    for euler_step in range(STEPS):
        mod_row = modulation[euler_step]

        def field_map(rows):
            return velocity(rows, mod_row, allowed, w_qkv, w_out, w_up, w_down, q_gain, k_gain)
        for probe_idx in range(PROBES):
            speed, tangent = jax.jvp(field_map, (latent,), (probe_signs[probe_idx],))
            change = change + lax.optimization_barrier(jnp.sum(probe_signs[probe_idx] * tangent, axis=1))
        latent = latent + step_size * speed
    density_change = -step_size * change / (PROBES * math.sqrt(D))
    return (latent, density_change)
```

```python
from functools import partial
import math

import jax
import jax.numpy as jnp
from jax import lax
from jax.experimental import pallas as pl
from jax.experimental.pallas import tpu as pltpu
from jax.sharding import PartitionSpec as P

HD = 128
BLK = 128
K_SEL = 8
STEPS = 2
NTP = 8
NZ = 8
NCTX = 16
W = 384
HALF = 64
ROWS = 256

EPS = 1e-06
NEG_BIG = -1e30
MESH = pl.DeviceIdType.MESH
F32 = jnp.float32
BF16 = jnp.bfloat16


def place():
    ctx, tp, core = lax.axis_index("ctx"), lax.axis_index("tp"), lax.axis_index("probe")
    return ctx, tp, core


def tp_at(offset):
    ctx, tp, core = place()
    return (ctx, lax.rem(tp + offset + NTP, NTP), core)


def sibling():
    ctx, tp, core = place()
    return (ctx, tp, 1 - core)


def ctx_at(block):
    _, tp, core = place()
    return (block, tp, core)


def greet(devices):
    barrier = pltpu.get_barrier_semaphore()
    for device in devices:
        pl.semaphore_signal(barrier, inc=1, device_id=device, device_id_type=MESH)
    pl.semaphore_wait(barrier, len(devices))


def remote(src, dst, send_sem, recv_sem, device):
    return pltpu.make_async_remote_copy(
        src_ref=src,
        dst_ref=dst,
        send_sem=send_sem,
        recv_sem=recv_sem,
        device_id=device,
        device_id_type=MESH,
    )


def feature_cols(owner):
    return pl.ds(pl.multiple_of(owner * W, 128), W)


def norm_kernel(lat, tan, shift, stretch, out, stat, s_send, s_recv, x_send, x_recv, f_send, f_recv):
    _, tp, core = place()
    rows_sent = pl.ds(pl.multiple_of(core * HALF, HALF), 3 * HALF)
    full = float(W * NTP)
    greet([tp_at(i) for i in range(1, NTP)] + [sibling()])
    rows, tangent = lat[...], tan[...]
    sums = [
        jnp.sum(rows, 1, keepdims=True),
        jnp.sum(rows * rows, 1, keepdims=True),
        jnp.sum(tangent, 1, keepdims=True),
        jnp.sum(rows * tangent, 1, keepdims=True),
    ]
    lane = lax.broadcasted_iota(jnp.int32, (BLK, BLK), 1)
    packed = jnp.zeros((BLK, BLK), F32)
    for n, column in enumerate(sums):
        packed = jnp.where(lane == n, column, packed)
    stat[tp] = packed.T[0:8]
    copies = []
    for i in range(1, NTP):
        copy = remote(stat.at[tp], stat.at[tp], s_send.at[i], s_recv.at[i], tp_at(i))
        copy.start()
        copies.append(copy)
    for i in range(1, NTP):
        source = lax.rem(tp - i + NTP, NTP)
        remote(stat.at[source], stat.at[source], s_send.at[i], s_recv.at[i], tp_at(i)).wait_recv()
    total = stat[0]
    for n in range(1, NTP):
        total = total + stat[n]
    total = jnp.concatenate([total, jnp.zeros((BLK - 8, BLK), F32)], axis=0).T * (1.0 / full)
    row_mean, row_sq, tan_mean, tan_sq = (total[:, n : n + 1] for n in range(4))
    row_var = row_sq - row_mean * row_mean
    tan_var = 2.0 * (tan_sq - row_mean * tan_mean)
    inv_std = lax.rsqrt(row_var + EPS)
    centred = rows - row_mean
    gain = 1.0 + stretch[...]
    normed = (centred * inv_std * gain + shift[...]).astype(BF16)
    tan_normed = (tangent - tan_mean) * inv_std - 0.5 * centred * (
        inv_std * inv_std * inv_std * tan_var
    )
    mine = feature_cols(tp)
    out[0:HALF, mine] = normed[0:HALF]
    out[HALF : 3 * HALF, mine] = (tan_normed * gain).astype(BF16)
    out[3 * HALF : ROWS, mine] = normed[HALF:BLK]
    for i in range(1, NTP):
        copy = remote(
            out.at[rows_sent, mine], out.at[rows_sent, mine], x_send.at[i], x_recv.at[i], tp_at(i)
        )
        copy.start()
        copies.append(copy)
    shared = pl.ds(pl.multiple_of(core * 3 * HALF, HALF), HALF)
    other = pl.ds(pl.multiple_of((1 - core) * 3 * HALF, HALF), HALF)
    for i in range(1, NTP):
        cols = feature_cols(lax.rem(tp - i + NTP, NTP))
        here = out.at[rows_sent, cols]
        remote(here, here, x_send.at[i], x_recv.at[i], tp_at(i)).wait_recv()
        piece = out.at[shared, cols]
        copy = remote(piece, piece, f_send.at[i], f_recv.at[i], sibling())
        copy.start()
        copies.append(copy)
    for i in range(1, NTP):
        cols = feature_cols(lax.rem(tp - i + NTP, NTP))
        piece = out.at[other, cols]
        remote(piece, piece, f_send.at[i], f_recv.at[i], sibling()).wait_recv()
    for copy in copies:
        copy.wait_send()


def norm_gather(lat, tan, shift, stretch):
    sems = [pltpu.SemaphoreType.DMA((NTP,)) for _ in range(6)]
    return pl.pallas_call(
        norm_kernel,
        out_shape=jax.ShapeDtypeStruct((ROWS, W * NTP), BF16),
        in_specs=[pl.BlockSpec(memory_space=pltpu.VMEM)] * 4,
        out_specs=pl.BlockSpec(memory_space=pltpu.VMEM),
        scratch_shapes=[pltpu.VMEM((NTP, 8, BLK), F32)] + sems,
        compiler_params=pltpu.CompilerParams(collective_id=1, has_side_effects=True),
        name="norm_gather",
    )(lat, tan, shift, stretch)


def ring_devices():
    ctx, _, _ = place()
    z, h = lax.rem(ctx, NZ), lax.div(ctx, NZ)
    right = h * NZ + lax.rem(z + 1, NZ)
    left = h * NZ + lax.rem(z + NZ - 1, NZ)
    across = (1 - h) * NZ + z
    return ctx_at(right), ctx_at(left), ctx_at(across)


def ring_gather(own, passed, given, sems):
    send, recv, f_send, f_recv = sems
    ctx, _, _ = place()
    z, h = lax.rem(ctx, NZ), lax.div(ctx, NZ)
    right, left, across = ring_devices()
    copies = []

    def push(block, n, device):
        copy = remote(own(block), own(block), send.at[n], recv.at[n], device)
        copy.start()
        copies.append(copy)

    def arrive(block, n):
        remote(own(block), own(block), send.at[n], recv.at[n], across).wait_recv()
        copy = remote(passed(block), passed(block), f_send.at[n], f_recv.at[n], sibling())
        copy.start()
        copies.append(copy)

    def at(row, step):
        return row * NZ + lax.rem(z + step + NZ, NZ)

    push(ctx, 0, across)
    push(ctx, 1, right)
    push(ctx, 8, left)
    arrive(at(1 - h, 0), 0)
    push(at(1 - h, 0), 5, right)
    push(at(1 - h, 0), 11, left)
    taken = [(at(1 - h, 0), 0)]
    for s in range(1, 5):
        for row, step, base, reach, device in (
            (h, -s, 0, 4, right),
            (h, s, 7, 3, left),
            (1 - h, -s, 4, 3, right),
            (1 - h, s, 10, 4, left),
        ):
            if s <= reach:
                block = at(row, step)
                arrive(block, base + s)
                taken.append((block, base + s))
                if s < reach:
                    push(block, base + s + 1, device)
    for block, n in taken:
        remote(given(block), given(block), f_send.at[n], f_recv.at[n], sibling()).wait_recv()
    for copy in copies:
        copy.wait_send()


def ring_sems():
    return [pltpu.SemaphoreType.DMA((15,)) for _ in range(4)]


def kv_kernel(mine, out, *sems):
    ctx, _, core = place()
    right, left, across = ring_devices()
    greet([right, left, across, sibling()])
    out[ctx] = mine[...]
    ring_gather(
        lambda block: out.at[block, pl.ds(core, 3)],
        lambda block: out.at[block, pl.ds(core * 3, 1)],
        lambda block: out.at[block, pl.ds((1 - core) * 3, 1)],
        sems,
    )


def kv_gather(mine):
    return pl.pallas_call(
        kv_kernel,
        out_shape=jax.ShapeDtypeStruct((NCTX,) + mine.shape, mine.dtype),
        in_specs=[pl.BlockSpec(memory_space=pltpu.VMEM)],
        out_specs=pl.BlockSpec(memory_space=pltpu.VMEM),
        scratch_shapes=ring_sems(),
        compiler_params=pltpu.CompilerParams(collective_id=2, has_side_effects=True),
        name="kv_gather",
    )(mine)


def weight_kernel(mine, out, *sems):
    ctx, _, core = place()
    right, left, across = ring_devices()
    greet([right, left, across, sibling()])
    out[0, ctx] = mine[0]
    out[1, ctx] = mine[1]
    ring_gather(
        lambda block: out.at[core, block],
        lambda block: out.at[core, block],
        lambda block: out.at[1 - core, block],
        sems,
    )


def weight_gather(mine):
    return pl.pallas_call(
        weight_kernel,
        out_shape=jax.ShapeDtypeStruct((2, NCTX) + mine.shape[1:], mine.dtype),
        in_specs=[pl.BlockSpec(memory_space=pltpu.VMEM)],
        out_specs=pl.BlockSpec(memory_space=pltpu.VMEM),
        scratch_shapes=ring_sems(),
        compiler_params=pltpu.CompilerParams(collective_id=3, has_side_effects=True),
        name="weight_gather",
    )(mine)


def reduce_kernel(part, out, got, r_send, r_recv, p_sem):
    _, tp, core = place()
    rows_sent = pl.ds(pl.multiple_of(core * HALF, HALF), 3 * HALF)
    greet([tp_at(i) for i in range(1, NTP)] + [sibling()])
    copies = []
    for i in range(1, NTP):
        cols = feature_cols(lax.rem(tp + i, NTP))
        copy = remote(part.at[rows_sent, cols], got.at[i], r_send.at[i], r_recv.at[i], tp_at(i))
        copy.start()
        copies.append(copy)
    total = part[rows_sent, feature_cols(tp)].astype(F32)
    for i in range(1, NTP):
        remote(got.at[i], got.at[i], r_send.at[i], r_recv.at[i], tp_at(i)).wait_recv()
        total = total + got[i].astype(F32)
    out[rows_sent] = total
    piece = out.at[pl.ds(pl.multiple_of(core * 3 * HALF, HALF), HALF)]
    other = out.at[pl.ds(pl.multiple_of((1 - core) * 3 * HALF, HALF), HALF)]
    copy = remote(piece, piece, p_sem.at[0], p_sem.at[1], sibling())
    copy.start()
    remote(other, other, p_sem.at[0], p_sem.at[1], sibling()).wait_recv()
    copies.append(copy)
    for copy in copies:
        copy.wait_send()


def reduce_parts(part):
    return pl.pallas_call(
        reduce_kernel,
        out_shape=jax.ShapeDtypeStruct((ROWS, W), F32),
        in_specs=[pl.BlockSpec(memory_space=pltpu.VMEM)],
        out_specs=pl.BlockSpec(memory_space=pltpu.VMEM),
        scratch_shapes=[
            pltpu.VMEM((NTP, 3 * HALF, W), BF16),
            pltpu.SemaphoreType.DMA((NTP,)),
            pltpu.SemaphoreType.DMA((NTP,)),
            pltpu.SemaphoreType.DMA((2,)),
        ],
        compiler_params=pltpu.CompilerParams(collective_id=4, has_side_effects=True),
        name="reduce_parts",
    )(part)


def primal_rows(rows):
    return jnp.concatenate([rows[0:HALF], rows[3 * HALF : ROWS]], axis=0)


def tangent_rows(rows):
    return rows[HALF : 3 * HALF]


def mixed_rows(primal, tangent):
    return jnp.concatenate([primal[0:HALF], tangent, primal[HALF:BLK]], axis=0)


def head_rms(projected, tan_projected, head_gain):
    row_count = projected.shape[0]
    heads_local = head_gain.shape[0] // HD
    head_view = projected.reshape(row_count, heads_local, HD)
    tan_view = tan_projected.reshape(row_count, heads_local, HD)
    gain_view = head_gain.reshape(heads_local, HD)
    inv_std = lax.rsqrt(jnp.mean(head_view * head_view, axis=-1, keepdims=True) + EPS)
    tan_inv = -inv_std * inv_std * inv_std * jnp.mean(head_view * tan_view, axis=-1, keepdims=True)
    result = (head_view * inv_std * gain_view).astype(BF16)
    tan_result = ((tan_view * inv_std + head_view * tan_inv) * gain_view).astype(BF16)
    return (result, tan_result)


def attend(query, kv, pattern):
    q_rows, dq_rows = query
    chosen = pattern[0]
    valid = (jnp.arange(K_SEL) == 0) | (chosen != chosen[0])
    key_mask = jnp.repeat(valid, BLK)[None, None, :]
    listed = jnp.take(kv, chosen, axis=0)

    def member(n):
        return listed[:, n].reshape(K_SEL * BLK, W // HD, HD)

    k_rows, dk_rows, dv_rows, v_rows = (member(n) for n in range(4))
    scale = 1.0 / math.sqrt(HD)
    dot = partial(jnp.einsum, preferred_element_type=F32)
    scores = dot("qhd,khd->hqk", q_rows, k_rows) * scale
    tan_scores = (
        dot("qhd,khd->hqk", dq_rows, k_rows) + dot("qhd,khd->hqk", q_rows, dk_rows)
    ) * scale
    scores = jnp.where(key_mask, scores, NEG_BIG)
    weights = jnp.where(key_mask, jnp.exp(scores - jnp.max(scores, 2, keepdims=True)), 0.0)
    weighted = weights * tan_scores
    total = jnp.sum(weights, 2)[:, :, None]
    tan_total = jnp.sum(weighted, 2)[:, :, None]
    weights, weighted = weights.astype(BF16), weighted.astype(BF16)
    output = dot("hqk,khd->hqd", weights, v_rows) / total
    tan_output = (
        dot("hqk,khd->hqd", weights, dv_rows) + dot("hqk,khd->hqd", weighted, v_rows)
    ) / total - (tan_total / total) * output

    def flat(rows):
        return rows.transpose(1, 0, 2).reshape(BLK, W).astype(BF16)

    return flat(output), flat(tan_output)


def local(latent, probes, modulation, pattern, w_qkv, w_out, w_up, w_down, q_gain, k_gain):
    row_count, local_width = latent.shape
    full_width = local_width * lax.axis_size("tp")
    feature_start = lax.axis_index("tp") * local_width
    step_size = 1.0 / STEPS
    signs = 2.0 * probes[0].astype(F32) - 1.0
    weights = weight_gather(jnp.stack([w_up, w_down.T]))
    up_full = weights[0].reshape(full_width, -1)
    down_full = weights[1].reshape(full_width, -1)
    gelu_tanh = partial(jax.nn.gelu, approximate=True)
    change = jnp.zeros((row_count,), F32)
    for euler_step in range(STEPS):
        mod_local = lax.dynamic_slice_in_dim(modulation[euler_step], feature_start, local_width, 1)
        stacked = norm_gather(latent, signs, mod_local[0:1], mod_local[1:2])
        projected = jnp.einsum("rd,dcf->crf", stacked, w_qkv, preferred_element_type=F32)
        q_rows, dq_rows = head_rms(primal_rows(projected[0]), tangent_rows(projected[0]), q_gain)
        k_rows, dk_rows = head_rms(primal_rows(projected[1]), tangent_rows(projected[1]), k_gain)
        v_rows = primal_rows(projected[2]).astype(BF16)
        dv_rows = tangent_rows(projected[2]).astype(BF16)
        kv = kv_gather(
            jnp.stack([k_rows.reshape(BLK, W), dk_rows.reshape(BLK, W), dv_rows, v_rows])
        )
        attended, tan_attended = attend((q_rows, dq_rows), kv, pattern)
        pre_hidden = jnp.dot(stacked, up_full, preferred_element_type=F32)
        hidden, tan_hidden = jax.jvp(
            gelu_tanh, (primal_rows(pre_hidden),), (tangent_rows(pre_hidden),)
        )
        attn_rows = mixed_rows(attended, tan_attended)
        mlp_rows = mixed_rows(hidden.astype(BF16), tan_hidden.astype(BF16))
        parts = jnp.dot(attn_rows, w_out, preferred_element_type=F32) + jnp.einsum(
            "rf,df->rd", mlp_rows, down_full, preferred_element_type=F32
        )
        summed = reduce_parts(parts.astype(BF16))
        speed = mod_local[2] * primal_rows(summed)
        tan_speed = mod_local[2] * tangent_rows(summed)
        change = change + jnp.sum(signs * tan_speed, axis=1)
        latent = latent + step_size * speed
    total_change = lax.psum(change, ("tp", "probe"))
    density_change = -step_size * total_change / (lax.axis_size("probe") * math.sqrt(full_width))
    return (latent, density_change)


def solution(mesh):
    return jax.shard_map(
        local,
        mesh=mesh,
        in_specs=(
            P("ctx", "tp"),
            P("probe", "ctx", "tp"),
            P(),
            P("ctx", None),
            P(None, None, "tp"),
            P("tp", None),
            P("ctx", "tp"),
            P("tp", "ctx"),
            P("tp"),
            P("tp"),
        ),
        out_specs=(P("ctx", "tp"), P("ctx")),
        check_vma=False,
    )
```

```python
from functools import partial
import math

import jax
import jax.numpy as jnp
from jax import lax
from jax.experimental import pallas as pl
from jax.experimental.pallas import tpu as pltpu
from jax.sharding import PartitionSpec as P

HD = 128
BLK = 128
K_SEL = 8
STEPS = 2
NTP = 8
NZ = 8
NCTX = 16
W = 384
D = 3072
HEADS = 3
UNITS = 768
SHARD = 192
HALF = 64
ROWS = 256

EPS = 1e-06
NEG_BIG = -1e30
MESH = pl.DeviceIdType.MESH
F32 = jnp.float32
BF16 = jnp.bfloat16


def place():
    return lax.axis_index("ctx"), lax.axis_index("tp"), lax.axis_index("probe")


def tp_at(offset):
    ctx, tp, core = place()
    return (ctx, lax.rem(tp + offset + NTP, NTP), core)


def sibling():
    ctx, tp, core = place()
    return (ctx, tp, 1 - core)


def ctx_at(block):
    _, tp, core = place()
    return (block, tp, core)


def ring_devices():
    ctx, _, _ = place()
    z, h = lax.rem(ctx, NZ), lax.div(ctx, NZ)
    right = h * NZ + lax.rem(z + 1, NZ)
    left = h * NZ + lax.rem(z + NZ - 1, NZ)
    across = (1 - h) * NZ + z
    return ctx_at(right), ctx_at(left), ctx_at(across)


def greet(devices):
    barrier = pltpu.get_barrier_semaphore()
    for device in devices:
        pl.semaphore_signal(barrier, inc=1, device_id=device, device_id_type=MESH)
    pl.semaphore_wait(barrier, len(devices))


def remote(src, dst, send_sem, recv_sem, device):
    return pltpu.make_async_remote_copy(
        src_ref=src,
        dst_ref=dst,
        send_sem=send_sem,
        recv_sem=recv_sem,
        device_id=device,
        device_id_type=MESH,
    )


def feature_cols(owner):
    return pl.ds(pl.multiple_of(owner * W, 128), W)


def half_rows(core):
    return pl.ds(pl.multiple_of(core * 3 * HALF, HALF), HALF)


class Ring:
    def __init__(self, own, passed, given, sems):
        self.own, self.passed, self.given = own, passed, given
        self.send, self.recv, self.f_send, self.f_recv = sems
        ctx, _, _ = place()
        z, h = lax.rem(ctx, NZ), lax.div(ctx, NZ)
        self.ctx = ctx
        self.right, self.left, self.across = ring_devices()
        self.copies, self.taken = [], []

        def at(row, step):
            return row * NZ + lax.rem(z + step + NZ, NZ)

        self.beside = at(1 - h, 0)
        self.todo = [(self.beside, 0, ((5, self.right), (11, self.left)))]
        for s in range(1, 5):
            for row, step, base, reach, device in (
                (h, -s, 0, 4, self.right),
                (h, s, 7, 3, self.left),
                (1 - h, -s, 4, 3, self.right),
                (1 - h, s, 10, 4, self.left),
            ):
                if s <= reach:
                    onward = ((base + s + 1, device),) if s < reach else ()
                    self.todo.append((at(row, step), base + s, onward))

    def push(self, block, n, device):
        copy = remote(self.own(block), self.own(block), self.send.at[n], self.recv.at[n], device)
        copy.start()
        self.copies.append(copy)

    def start(self):
        self.push(self.ctx, 0, self.across)
        self.push(self.ctx, 1, self.right)
        self.push(self.ctx, 8, self.left)

    def advance(self, count=1):
        for _ in range(count):
            if not self.todo:
                return
            block, n, onward = self.todo.pop(0)
            mine = self.own(block)
            remote(mine, mine, self.send.at[n], self.recv.at[n], self.across).wait_recv()
            for later, device in onward:
                self.push(block, later, device)
            piece = self.passed(block)
            copy = remote(piece, piece, self.f_send.at[n], self.f_recv.at[n], sibling())
            copy.start()
            self.copies.append(copy)
            self.taken.append((block, n))

    def finish(self):
        self.advance(len(self.todo))
        for block, n in self.taken:
            piece = self.given(block)
            remote(piece, piece, self.f_send.at[n], self.f_recv.at[n], sibling()).wait_recv()

    def drain(self):
        for copy in self.copies:
            copy.wait_send()


def gelu_pair(pre, tan_pre):
    c = math.sqrt(2.0 / math.pi)
    square = pre * pre
    t = jnp.tanh(c * (pre + 0.044715 * (square * pre)))
    half = 0.5 * (1.0 + t)
    slope = half + 0.5 * pre * (1.0 - t * t) * (c * (1.0 + 3.0 * 0.044715 * square))
    return pre * half, slope * tan_pre


def columns_to_rows(columns):
    lane = lax.broadcasted_iota(jnp.int32, (BLK, BLK), 1)
    packed = jnp.zeros((BLK, BLK), F32)
    for n, column in enumerate(columns):
        packed = jnp.where(lane == n, column, packed)
    return packed.T[0:8]


def rows_to_columns(rows):
    return jnp.concatenate([rows, jnp.zeros((BLK - 8, BLK), F32)], axis=0).T


def body(
    lat, probes, mod, gains, pattern, wqkv_hbm, wout_hbm, wup_hbm, wdn_hbm,
    lat_out, dens_out,
    wqkv, wout, wmlp, kv_first, kv_second, x, signs, proj, queries, hid, attn, acc, part, got, tot, stat, dens,
    w_sem, s_send, s_recv, x_send, x_recv, f_send, f_recv, r_send, r_recv, p_send, p_recv,
    d_send, d_recv, *ring_sems,
):
    ctx, tp, core = place()
    mine = feature_cols(tp)
    rows_sent = pl.ds(pl.multiple_of(core * HALF, HALF), 3 * HALF)
    full = float(D)
    shard = pl.ds(pl.multiple_of(ctx * SHARD, 64), SHARD)
    loads = [
        pltpu.make_async_copy(wup_hbm, wmlp.at[0, shard], w_sem.at[0]),
        pltpu.make_async_copy(wdn_hbm, wmlp.at[1, shard], w_sem.at[1]),
        pltpu.make_async_copy(wqkv_hbm.at[1], wqkv.at[:, 0:W], w_sem.at[2]),
        pltpu.make_async_copy(wqkv_hbm.at[2], wqkv.at[:, W : 2 * W], w_sem.at[3]),
        pltpu.make_async_copy(wqkv_hbm.at[0], wqkv.at[:, 2 * W : 3 * W], w_sem.at[4]),
        pltpu.make_async_copy(wout_hbm, wout, w_sem.at[5]),
    ]
    for load in loads:
        load.start()
    signs[...] = 2.0 * probes[...].astype(F32) - 1.0
    lat_out[...] = lat[...]
    right, left, across = ring_devices()
    greet([tp_at(i) for i in range(1, NTP)] + [right, left, across, sibling()])

    def block_rows(block):
        return pl.ds(pl.multiple_of(block * SHARD, 64), SHARD)

    weight_ring = Ring(
        lambda block: wmlp.at[core, block_rows(block)],
        lambda block: wmlp.at[core, block_rows(block)],
        lambda block: wmlp.at[1 - core, block_rows(block)],
        [sems.at[STEPS] for sems in ring_sems],
    )
    loads[0].wait()
    loads[1].wait()
    weight_ring.start()
    change = jnp.zeros((BLK, 1), F32)

    for step in range(STEPS):
        copies = []
        kv = (kv_first, kv_second)[step]
        rows, tangent = lat_out[...], signs[...]
        stat[tp] = columns_to_rows(
            [
                jnp.sum(rows, 1, keepdims=True),
                jnp.sum(rows * rows, 1, keepdims=True),
                jnp.sum(tangent, 1, keepdims=True),
                jnp.sum(rows * tangent, 1, keepdims=True),
            ]
        )
        for i in range(1, NTP):
            copy = remote(
                stat.at[tp], stat.at[tp], s_send.at[step, i], s_recv.at[step, i], tp_at(i)
            )
            copy.start()
            copies.append(copy)
        for i in range(1, NTP):
            there = stat.at[lax.rem(tp - i + NTP, NTP)]
            remote(there, there, s_send.at[step, i], s_recv.at[step, i], tp_at(i)).wait_recv()
        total = stat[0]
        for n in range(1, NTP):
            total = total + stat[n]
        total = rows_to_columns(total) * (1.0 / full)
        row_mean, row_sq, tan_mean, tan_sq = (total[:, n : n + 1] for n in range(4))
        row_var = row_sq - row_mean * row_mean
        tan_var = 2.0 * (tan_sq - row_mean * tan_mean)
        inv_std = lax.rsqrt(row_var + EPS)
        centred = rows - row_mean
        shift, gain = mod[3 * step : 3 * step + 1], 1.0 + mod[3 * step + 1 : 3 * step + 2]
        normed = (centred * inv_std * gain + shift).astype(BF16)
        tan_normed = (tangent - tan_mean) * inv_std - 0.5 * centred * (
            inv_std * inv_std * inv_std * tan_var
        )
        x[0:HALF, mine] = normed[0:HALF]
        x[HALF : 3 * HALF, mine] = (tan_normed * gain).astype(BF16)
        x[3 * HALF : ROWS, mine] = normed[HALF:BLK]
        for i in range(1, NTP):
            here = x.at[rows_sent, mine]
            copy = remote(here, here, x_send.at[step, i], x_recv.at[step, i], tp_at(i))
            copy.start()
            copies.append(copy)
        if step == 0:
            weight_ring.advance(2)
        for i in range(1, NTP):
            cols = feature_cols(lax.rem(tp - i + NTP, NTP))
            here = x.at[rows_sent, cols]
            remote(here, here, x_send.at[step, i], x_recv.at[step, i], tp_at(i)).wait_recv()
            piece = x.at[half_rows(core), cols]
            copy = remote(piece, piece, f_send.at[step, i], f_recv.at[step, i], sibling())
            copy.start()
            copies.append(copy)
            if step == 0 and i in (2, 4, 6):
                weight_ring.advance(1)
        for i in range(1, NTP):
            piece = x.at[half_rows(1 - core), feature_cols(lax.rem(tp - i + NTP, NTP))]
            remote(piece, piece, f_send.at[step, i], f_recv.at[step, i], sibling()).wait_recv()
        if step == 0:
            for load in loads[2:]:
                load.wait()

        def head_pair(column, gain_row, h):
            view = proj[:, column + h * HD : column + (h + 1) * HD]
            primal = jnp.concatenate([view[0:HALF], view[3 * HALF : ROWS]], axis=0)
            tan = view[HALF : 3 * HALF]
            gain_view = gains[gain_row : gain_row + 1, h * HD : (h + 1) * HD]
            inv = lax.rsqrt(jnp.mean(primal * primal, 1, keepdims=True) + EPS)
            tan_inv = -inv * inv * inv * jnp.mean(primal * tan, 1, keepdims=True)
            return (
                (primal * inv * gain_view).astype(BF16),
                ((tan * inv + primal * tan_inv) * gain_view).astype(BF16),
            )

        def project(start, stop):
            proj[:, start:stop] = jnp.dot(
                x[...], wqkv[:, start:stop], preferred_element_type=F32
            )

        for n in range(3):
            project(256 * n, 256 * (n + 1))
        if step == 0:
            weight_ring.advance(1)
        for h in range(HEADS):
            cols = slice(h * HD, (h + 1) * HD)
            key, tan_key = head_pair(0, 1, h)
            kv[ctx, 0, :, cols] = key
            kv[ctx, 1, :, cols] = tan_key
        kv[ctx, 2] = proj[HALF : 3 * HALF, W : 2 * W].astype(BF16)
        kv[ctx, 3, 0:HALF] = proj[0:HALF, W : 2 * W].astype(BF16)
        kv[ctx, 3, HALF:BLK] = proj[3 * HALF : ROWS, W : 2 * W].astype(BF16)
        kv_ring = Ring(
            lambda block, kv=kv: kv.at[block, pl.ds(core, 3)],
            lambda block, kv=kv: kv.at[block, pl.ds(core * 3, 1)],
            lambda block, kv=kv: kv.at[block, pl.ds((1 - core) * 3, 1)],
            [sems.at[step] for sems in ring_sems],
        )
        kv_ring.start()
        if step == 0:
            weight_ring.advance(2)
        project(768, 1152)
        for h in range(HEADS):
            query, tan_query = head_pair(768, 0, h)
            queries[0:BLK, h * HD : (h + 1) * HD] = query
            queries[BLK:ROWS, h * HD : (h + 1) * HD] = tan_query
        if step == 0:
            while weight_ring.todo:
                weight_ring.advance(2)
                kv_ring.advance(1)
            weight_ring.finish()
        else:
            kv_ring.advance(2)
        for n in range(3):
            cols = slice(256 * n, 256 * (n + 1))
            pre = jnp.dot(x[...], wmlp[0, :, cols], preferred_element_type=F32)
            primal = jnp.concatenate([pre[0:HALF], pre[3 * HALF : ROWS]], axis=0)
            hidden, tan_hidden = gelu_pair(primal, pre[HALF : 3 * HALF])
            hidden = hidden.astype(BF16)
            hid[0:HALF, cols] = hidden[0:HALF]
            hid[HALF : 3 * HALF, cols] = tan_hidden.astype(BF16)
            hid[3 * HALF : ROWS, cols] = hidden[HALF:BLK]
            kv_ring.advance(1)
        for n in range(4):
            cols = slice(768 * n, 768 * (n + 1))
            acc[:, cols] = lax.dot_general(
                hid[...],
                wmlp[1, cols, :],
                (((1,), (1,)), ((), ())),
                preferred_element_type=F32,
            )
            kv_ring.advance(2)
        kv_ring.finish()
        first = pattern[0, 0]
        listed = [pattern[0, j] for j in range(K_SEL)]
        penalty = [
            jnp.where(listed[j] == first, NEG_BIG, 0.0).astype(F32) if j else None
            for j in range(K_SEL)
        ]
        scale = 1.0 / math.sqrt(HD)
        contract = (((1,), (1,)), ((), ()))
        for h in range(HEADS):
            cols = slice(h * HD, (h + 1) * HD)
            pair = queries[:, cols]
            scores, tan_scores = [], []
            for j in range(K_SEL):
                key, tan_key = kv[listed[j], 0, :, cols], kv[listed[j], 1, :, cols]
                both = lax.dot_general(pair, key, contract, preferred_element_type=F32) * scale
                cross = lax.dot_general(
                    pair[0:BLK], tan_key, contract, preferred_element_type=F32
                )
                score = both[0:BLK]
                scores.append(score + penalty[j] if j else score)
                tan_scores.append(both[BLK:ROWS] + cross * scale)
            top = scores[0]
            for j in range(1, K_SEL):
                top = jnp.maximum(top, scores[j])
            top = jnp.max(top, 1, keepdims=True)
            out = jnp.zeros((ROWS, 2 * HD), F32)
            weight_sum, tan_sum = jnp.zeros((BLK, BLK), F32), jnp.zeros((BLK, BLK), F32)
            for j in range(K_SEL):
                weights = jnp.exp(scores[j] - top)
                weighted = weights * tan_scores[j]
                weight_sum, tan_sum = weight_sum + weights, tan_sum + weighted
                left_side = jnp.concatenate([weights, weighted], axis=0).astype(BF16)
                values = jnp.concatenate(
                    [kv[listed[j], 3, :, cols], kv[listed[j], 2, :, cols]], axis=1
                )
                out = out + jnp.dot(left_side, values, preferred_element_type=F32)
            inv = 1.0 / jnp.sum(weight_sum, 1, keepdims=True)
            ratio = jnp.sum(tan_sum, 1, keepdims=True) * inv
            output = out[0:BLK, 0:HD] * inv
            tan_output = (out[0:BLK, HD : 2 * HD] + out[BLK:ROWS, 0:HD]) * inv - ratio * output
            output = output.astype(BF16)
            attn[0:HALF, cols] = output[0:HALF]
            attn[HALF : 3 * HALF, cols] = tan_output.astype(BF16)
            attn[3 * HALF : ROWS, cols] = output[HALF:BLK]
        for copy in copies:
            copy.wait_send()
        copies = []
        for i in range(1, NTP + 1):
            cols = feature_cols(lax.rem(tp + i, NTP))
            part[i % NTP] = (
                acc[:, cols] + jnp.dot(attn[...], wout[:, cols], preferred_element_type=F32)
            ).astype(BF16)
            if i < NTP:
                copy = remote(
                    part.at[i, rows_sent],
                    got.at[i],
                    r_send.at[step, i],
                    r_recv.at[step, i],
                    tp_at(i),
                )
                copy.start()
                copies.append(copy)
        total = part[0, rows_sent].astype(F32)
        for i in range(1, NTP):
            remote(
                got.at[i], got.at[i], r_send.at[step, i], r_recv.at[step, i], tp_at(i)
            ).wait_recv()
            total = total + got[i].astype(F32)
        tot[rows_sent] = total
        piece, other = tot.at[half_rows(core)], tot.at[half_rows(1 - core)]
        copy = remote(piece, piece, p_send.at[step], p_recv.at[step], sibling())
        copy.start()
        copies.append(copy)
        gate = mod[3 * step + 2 : 3 * step + 3]
        change = change + jnp.sum(
            signs[...] * (gate * tot[HALF : 3 * HALF]), axis=1, keepdims=True
        )
        remote(other, other, p_send.at[step], p_recv.at[step], sibling()).wait_recv()
        lat_out[0:HALF] += (1.0 / STEPS) * (gate * tot[0:HALF])
        lat_out[HALF:BLK] += (1.0 / STEPS) * (gate * tot[3 * HALF : ROWS])
        for copy in copies:
            copy.wait_send()
        kv_ring.drain()
        if step == 0:
            weight_ring.drain()

    copies = []
    dens[tp] = columns_to_rows([change])
    for i in range(1, NTP):
        copy = remote(dens.at[tp], dens.at[tp], d_send.at[i], d_recv.at[i], tp_at(i))
        copy.start()
        copies.append(copy)
    for i in range(1, NTP):
        there = dens.at[lax.rem(tp - i + NTP, NTP)]
        remote(there, there, d_send.at[i], d_recv.at[i], tp_at(i)).wait_recv()
    total = dens[0]
    for n in range(1, NTP):
        total = total + dens[n]
    dens[NTP] = total
    copy = remote(dens.at[NTP], dens.at[NTP + 1], d_send.at[0], d_recv.at[0], sibling())
    copy.start()
    remote(dens.at[NTP + 1], dens.at[NTP + 1], d_send.at[0], d_recv.at[0], sibling()).wait_recv()
    copies.append(copy)
    dens_out[...] = (dens[NTP] + dens[NTP + 1]) * (-1.0 / (STEPS * 2 * math.sqrt(full)))
    for copy in copies:
        copy.wait_send()


def local(latent, probes, modulation, pattern, w_qkv, w_out, w_up, w_down, q_gain, k_gain):
    start = lax.axis_index("tp") * W
    mod = lax.dynamic_slice_in_dim(modulation.reshape(3 * STEPS, D), start, W, 1)
    gains = jnp.stack([q_gain, k_gain])
    vmem, anywhere = pl.BlockSpec(memory_space=pltpu.VMEM), pl.BlockSpec(memory_space=pl.ANY)
    dma = pltpu.SemaphoreType.DMA
    latent_out, density = pl.pallas_call(
        body,
        out_shape=(
            jax.ShapeDtypeStruct((BLK, W), F32),
            jax.ShapeDtypeStruct((8, BLK), F32),
        ),
        in_specs=[vmem] * 4 + [pl.BlockSpec(memory_space=pltpu.SMEM)] + [anywhere] * 4,
        out_specs=(vmem, vmem),
        scratch_shapes=[
            pltpu.VMEM((D, 3 * W), BF16),
            pltpu.VMEM((W, D), BF16),
            pltpu.VMEM((2, D, UNITS), BF16),
            pltpu.VMEM((NCTX, 4, BLK, W), BF16),
            pltpu.VMEM((NCTX, 4, BLK, W), BF16),
            pltpu.VMEM((ROWS, D), BF16),
            pltpu.VMEM((BLK, W), F32),
            pltpu.VMEM((ROWS, 3 * W), F32),
            pltpu.VMEM((ROWS, W), BF16),
            pltpu.VMEM((ROWS, UNITS), BF16),
            pltpu.VMEM((ROWS, W), BF16),
            pltpu.VMEM((ROWS, D), F32),
            pltpu.VMEM((NTP, ROWS, W), BF16),
            pltpu.VMEM((NTP, 3 * HALF, W), BF16),
            pltpu.VMEM((ROWS, W), F32),
            pltpu.VMEM((NTP, 8, BLK), F32),
            pltpu.VMEM((NTP + 2, 8, BLK), F32),
            dma((6,)),
        ]
        + [dma((STEPS, NTP)) for _ in range(8)]
        + [dma((STEPS,)) for _ in range(2)]
        + [dma((NTP,)) for _ in range(2)]
        + [dma((STEPS + 1, 15)) for _ in range(4)],
        compiler_params=pltpu.CompilerParams(
            collective_id=1, has_side_effects=True, vmem_limit_bytes=60 * 1024 * 1024
        ),
        name="euler_steps",
    )(
        latent,
        probes[0],
        mod,
        gains,
        pattern,
        w_qkv.transpose(1, 0, 2),
        w_out,
        w_up,
        w_down.T,
    )
    return latent_out, density[0]


def solution(mesh):
    return jax.shard_map(
        local,
        mesh=mesh,
        in_specs=(
            P("ctx", "tp"),
            P("probe", "ctx", "tp"),
            P(),
            P("ctx", None),
            P(None, None, "tp"),
            P("tp", None),
            P("ctx", "tp"),
            P("tp", "ctx"),
            P("tp"),
            P("tp"),
        ),
        out_specs=(P("ctx", "tp"), P("ctx")),
        check_vma=False,
    )
```

```python
from functools import partial
import math

import jax
import jax.numpy as jnp
from jax import lax
from jax.experimental import pallas as pl
from jax.experimental.pallas import tpu as pltpu
from jax.sharding import PartitionSpec as P

HD = 128
BLK = 128
K_SEL = 8
STEPS = 2
NTP = 8
NZ = 8
NCTX = 16
W = 384
D = 3072
HEADS = 3
UNITS = 768
SHARD = 192
HALF = 64
ROWS = 256

EPS = 1e-06
NEG_BIG = -1e30
MESH = pl.DeviceIdType.MESH
F32 = jnp.float32
BF16 = jnp.bfloat16


def place():
    return lax.axis_index("ctx"), lax.axis_index("tp"), lax.axis_index("probe")


def tp_at(offset):
    ctx, tp, core = place()
    return (ctx, lax.rem(tp + offset + NTP, NTP), core)


def sibling():
    ctx, tp, core = place()
    return (ctx, tp, 1 - core)


def ctx_at(block):
    _, tp, core = place()
    return (block, tp, core)


def ring_devices():
    ctx, _, _ = place()
    z, h = lax.rem(ctx, NZ), lax.div(ctx, NZ)
    right = h * NZ + lax.rem(z + 1, NZ)
    left = h * NZ + lax.rem(z + NZ - 1, NZ)
    across = (1 - h) * NZ + z
    return ctx_at(right), ctx_at(left), ctx_at(across)


def greet(devices):
    barrier = pltpu.get_barrier_semaphore()
    for device in devices:
        pl.semaphore_signal(barrier, inc=1, device_id=device, device_id_type=MESH)
    pl.semaphore_wait(barrier, len(devices))


def remote(src, dst, send_sem, recv_sem, device):
    return pltpu.make_async_remote_copy(
        src_ref=src,
        dst_ref=dst,
        send_sem=send_sem,
        recv_sem=recv_sem,
        device_id=device,
        device_id_type=MESH,
    )


def feature_cols(owner):
    return pl.ds(pl.multiple_of(owner * W, 128), W)


def head_cols(owner):
    return pl.ds(pl.multiple_of(owner * HD, 128), HD)


def half_rows(core):
    return pl.ds(pl.multiple_of(core * 3 * HALF, HALF), HALF)


class Ring:
    def __init__(self, own, passed, given, sems):
        self.own, self.passed, self.given = own, passed, given
        self.send, self.recv, self.f_send, self.f_recv = sems
        ctx, _, core = place()
        z, h = lax.rem(ctx, NZ), lax.div(ctx, NZ)
        self.ctx = ctx
        right, left, across = ring_devices()
        turn = 1 - 2 * core
        ahead = ctx_at(h * NZ + lax.rem(z + turn + NZ, NZ))
        behind = ctx_at(h * NZ + lax.rem(z - turn + NZ, NZ))
        self.right, self.left, self.across, self.ahead, self.behind = right, left, across, ahead, behind
        self.copies, self.taken = [], []

        def at(row, step):
            return row * NZ + lax.rem(z + step + NZ, NZ)

        self.todo = [
            (at(1 - h, 0), 0, 0, ((5, right), (11, left))),
            (at(1 - h, 0), 1, 22, ()),
        ]
        for s in range(1, 5):
            for row, step, base, reach, device in (
                (h, -s, 0, 4, right),
                (h, s, 7, 3, left),
            ):
                if s <= reach:
                    onward = ((base + s + 1, device),) if s < reach else ()
                    self.todo.append((at(row, step), 0, base + s, onward))
            for step, base, y_base, reach, device in (
                (-s * turn, 14, 22, 4, ahead),
                (s * turn, 18, 26, 3, behind),
            ):
                if s <= reach:
                    onward = ((base + s + 1, device),) if s < reach else ()
                    onward = onward + ((y_base + s, across),)
                    self.todo.append((at(h, step), 1, base + s, onward))
            for row, step, base, reach, device in (
                (1 - h, -s, 4, 3, right),
                (1 - h, s, 10, 4, left),
            ):
                if s <= reach:
                    onward = ((base + s + 1, device),) if s < reach else ()
                    self.todo.append((at(row, step), 0, base + s, onward))
            self.todo.append((at(1 - h, -s * turn), 1, 22 + s, ()))
            if s <= 3:
                self.todo.append((at(1 - h, s * turn), 1, 26 + s, ()))

    def push(self, block, part, n, device):
        piece = self.own(block, part)
        copy = remote(piece, piece, self.send.at[n], self.recv.at[n], device)
        copy.start()
        self.copies.append(copy)

    def start(self):
        self.push(self.ctx, 0, 0, self.across)
        self.push(self.ctx, 0, 1, self.right)
        self.push(self.ctx, 0, 8, self.left)
        self.push(self.ctx, 1, 15, self.ahead)
        self.push(self.ctx, 1, 19, self.behind)
        self.push(self.ctx, 1, 22, self.across)

    def advance(self, count=1):
        for _ in range(count):
            if not self.todo:
                return
            block, part, n, onward = self.todo.pop(0)
            mine = self.own(block, part)
            remote(mine, mine, self.send.at[n], self.recv.at[n], self.across).wait_recv()
            for later, device in onward:
                self.push(block, part, later, device)
            piece = self.passed(block, part)
            copy = remote(piece, piece, self.f_send.at[n], self.f_recv.at[n], sibling())
            copy.start()
            self.copies.append(copy)
            self.taken.append((block, part, n))

    def finish(self):
        self.advance(len(self.todo))
        for block, part, n in self.taken:
            piece = self.given(block, part)
            remote(piece, piece, self.f_send.at[n], self.f_recv.at[n], sibling()).wait_recv()

    def drain(self):
        for copy in self.copies:
            copy.wait_send()


class Share:
    def __init__(self, piece, passed, given, sems, source=None):
        self.piece, self.passed, self.given = piece, passed, given
        self.send, self.recv, self.f_send, self.f_recv = sems
        self.tp = lax.axis_index("tp")
        self.source = source or (lambda i: piece(self.tp))
        self.copies = []
        self.next = 1

    def owner(self, i):
        return lax.rem(self.tp - i + NTP, NTP)

    def push(self):
        for i in range(1, NTP):
            copy = remote(
                self.source(i), self.piece(self.tp), self.send.at[i], self.recv.at[i], tp_at(i)
            )
            copy.start()
            self.copies.append(copy)

    def collect(self, count=NTP):
        while self.next < NTP and count:
            i, owner = self.next, self.owner(self.next)
            here = self.piece(owner)
            remote(here, here, self.send.at[i], self.recv.at[i], tp_at(i)).wait_recv()
            part = self.passed(owner)
            copy = remote(part, part, self.f_send.at[i], self.f_recv.at[i], sibling())
            copy.start()
            self.copies.append(copy)
            self.next, count = self.next + 1, count - 1

    def finish(self):
        self.collect()
        for i in range(1, NTP):
            part = self.given(self.owner(i))
            remote(part, part, self.f_send.at[i], self.f_recv.at[i], sibling()).wait_recv()

    def drain(self):
        for copy in self.copies:
            copy.wait_send()


def gelu_pair(pre, tan_pre):
    c = math.sqrt(2.0 / math.pi)
    square = pre * pre
    t = jnp.tanh(c * (pre + 0.044715 * (square * pre)))
    half = 0.5 * (1.0 + t)
    slope = half + 0.5 * pre * (1.0 - t * t) * (c * (1.0 + 3.0 * 0.044715 * square))
    return pre * half, slope * tan_pre


def columns_to_rows(columns):
    lane = lax.broadcasted_iota(jnp.int32, (BLK, BLK), 1)
    packed = jnp.zeros((BLK, BLK), F32)
    for n, column in enumerate(columns):
        packed = jnp.where(lane == n, column, packed)
    return packed.T[0:8]


def rows_to_columns(rows):
    return jnp.concatenate([rows, jnp.zeros((BLK - 8, BLK), F32)], axis=0).T


def body(
    lat, probes, mod, gains, pattern, wqkv_hbm, wout_hbm, wup_hbm, wdn_hbm,
    lat_out, dens_out,
    kv_0, kv_1, kv_2, kv_3, kv_4, kv_5,
    wqkv, wo, wmlp, x, xa_0, xa_1, xa_2, signs, proj, queries, hid, acc, part, got, tot, stat, dens,
    w_sem, s_send, s_recv, r_send, r_recv, p_send, p_recv, d_send, d_recv,
    *many_sems,
):
    ring_sems, share_sems = many_sems[:4], many_sems[4:]
    ctx, tp, core = place()
    mine = feature_cols(tp)
    rows_sent = pl.ds(pl.multiple_of(core * HALF, HALF), 3 * HALF)
    my_half = pl.ds(pl.multiple_of(core * HALF, HALF), HALF)
    other_half = pl.ds(pl.multiple_of((1 - core) * HALF, HALF), HALF)
    full = float(D)
    shard = pl.ds(pl.multiple_of(ctx * SHARD, 64), SHARD)
    loads = [
        pltpu.make_async_copy(wup_hbm, wmlp.at[0, shard], w_sem.at[0]),
        pltpu.make_async_copy(wdn_hbm, wmlp.at[1, shard], w_sem.at[1]),
        pltpu.make_async_copy(wqkv_hbm.at[1], wqkv.at[:, 0:W], w_sem.at[2]),
        pltpu.make_async_copy(wqkv_hbm.at[2], wqkv.at[:, W : 2 * W], w_sem.at[3]),
        pltpu.make_async_copy(wqkv_hbm.at[0], wqkv.at[:, 2 * W : 3 * W], w_sem.at[4]),
        pltpu.make_async_copy(wout_hbm.at[:, :, mine], wo.at[:, tp], w_sem.at[5]),
    ]
    for load in loads:
        load.start()
    signs[...] = 2.0 * probes[...].astype(F32) - 1.0
    lat_out[...] = lat[...]
    right, left, across = ring_devices()
    greet([tp_at(i) for i in range(1, NTP)] + [right, left, across, sibling()])

    def block_rows(block, part):
        return pl.ds(pl.multiple_of(block * SHARD + part * (SHARD // 2), 32), SHARD // 2)

    weight_ring = Ring(
        lambda block, part: wmlp.at[core, block_rows(block, part)],
        lambda block, part: wmlp.at[core, block_rows(block, part)],
        lambda block, part: wmlp.at[1 - core, block_rows(block, part)],
        [sems.at[STEPS * HEADS] for sems in ring_sems],
    )
    wout_share = Share(
        lambda owner: wo.at[:, owner, my_half],
        lambda owner: wo.at[:, owner, my_half],
        lambda owner: wo.at[:, owner, other_half],
        [sems.at[STEPS * (HEADS + 1)] for sems in share_sems],
        lambda i: wout_hbm.at[:, my_half, feature_cols(lax.rem(tp + i, NTP))],
    )
    loads[0].wait()
    loads[1].wait()
    weight_ring.start()
    change = jnp.zeros((BLK, 1), F32)

    for step in range(STEPS):
        copies = []
        kvs = (kv_0, kv_1, kv_2, kv_3, kv_4, kv_5)[HEADS * step : HEADS * (step + 1)]
        xas = (xa_0, xa_1, xa_2)
        rows, tangent = lat_out[...], signs[...]
        stat[tp] = columns_to_rows(
            [
                jnp.sum(rows, 1, keepdims=True),
                jnp.sum(rows * rows, 1, keepdims=True),
                jnp.sum(tangent, 1, keepdims=True),
                jnp.sum(rows * tangent, 1, keepdims=True),
            ]
        )
        for i in range(1, NTP):
            copy = remote(
                stat.at[tp], stat.at[tp], s_send.at[step, i], s_recv.at[step, i], tp_at(i)
            )
            copy.start()
            copies.append(copy)
        for i in range(1, NTP):
            there = stat.at[lax.rem(tp - i + NTP, NTP)]
            remote(there, there, s_send.at[step, i], s_recv.at[step, i], tp_at(i)).wait_recv()
        total = stat[0]
        for n in range(1, NTP):
            total = total + stat[n]
        total = rows_to_columns(total) * (1.0 / full)
        row_mean, row_sq, tan_mean, tan_sq = (total[:, n : n + 1] for n in range(4))
        row_var = row_sq - row_mean * row_mean
        tan_var = 2.0 * (tan_sq - row_mean * tan_mean)
        inv_std = lax.rsqrt(row_var + EPS)
        centred = rows - row_mean
        shift, gain = mod[3 * step : 3 * step + 1], 1.0 + mod[3 * step + 1 : 3 * step + 2]
        normed = (centred * inv_std * gain + shift).astype(BF16)
        tan_normed = (tangent - tan_mean) * inv_std - 0.5 * centred * (
            inv_std * inv_std * inv_std * tan_var
        )
        x[0:HALF, mine] = normed[0:HALF]
        x[HALF : 3 * HALF, mine] = (tan_normed * gain).astype(BF16)
        x[3 * HALF : ROWS, mine] = normed[HALF:BLK]
        x_share = Share(
            lambda owner: x.at[rows_sent, feature_cols(owner)],
            lambda owner: x.at[half_rows(core), feature_cols(owner)],
            lambda owner: x.at[half_rows(1 - core), feature_cols(owner)],
            [sems.at[step] for sems in share_sems],
        )
        x_share.push()
        if step == 0:
            weight_ring.advance(2)
            for _ in range(3):
                x_share.collect(2)
                weight_ring.advance(2)
        x_share.finish()
        if step == 0:
            for load in loads[2:]:
                load.wait()

        def head_pair(column, gain_row, h):
            view = proj[:, column + h * HD : column + (h + 1) * HD]
            primal = jnp.concatenate([view[0:HALF], view[3 * HALF : ROWS]], axis=0)
            tan = view[HALF : 3 * HALF]
            gain_view = gains[gain_row : gain_row + 1, h * HD : (h + 1) * HD]
            inv = lax.rsqrt(jnp.mean(primal * primal, 1, keepdims=True) + EPS)
            tan_inv = -inv * inv * inv * jnp.mean(primal * tan, 1, keepdims=True)
            return (
                (primal * inv * gain_view).astype(BF16),
                ((tan * inv + primal * tan_inv) * gain_view).astype(BF16),
            )

        def project(start, stop):
            proj[:, start:stop] = jnp.dot(
                x[...], wqkv[:, start:stop], preferred_element_type=F32
            )

        def own_block(h):
            kv = kvs[h]
            key, tan_key = head_pair(0, 1, h)
            cols = slice(W + h * HD, W + (h + 1) * HD)
            kv[ctx, 0] = key
            kv[ctx, 1] = tan_key
            kv[ctx, 2] = proj[HALF : 3 * HALF, cols].astype(BF16)
            kv[ctx, 3, 0:HALF] = proj[0:HALF, cols].astype(BF16)
            kv[ctx, 3, HALF:BLK] = proj[3 * HALF : ROWS, cols].astype(BF16)

        def part_rows(part):
            return slice(part * HALF, (part + 1) * HALF)

        rings = [
            Ring(
                lambda block, part, kv=kv: kv.at[block, pl.ds(core, 3), part_rows(part)],
                lambda block, part, kv=kv: kv.at[block, pl.ds(core * 3, 1), part_rows(part)],
                lambda block, part, kv=kv: kv.at[block, pl.ds((1 - core) * 3, 1), part_rows(part)],
                [sems.at[step * HEADS + h] for sems in ring_sems],
            )
            for h, kv in enumerate(kvs)
        ]
        shares = [
            Share(
                lambda owner, xa=xa: xa.at[rows_sent, head_cols(owner)],
                lambda owner, xa=xa: xa.at[half_rows(core), head_cols(owner)],
                lambda owner, xa=xa: xa.at[half_rows(1 - core), head_cols(owner)],
                [sems.at[STEPS + step * HEADS + h] for sems in share_sems],
            )
            for h, xa in enumerate(xas)
        ]
        for n in range(3):
            project(256 * n, 256 * (n + 1))
        own_block(0)
        rings[0].start()
        if step == 0:
            weight_ring.advance(4)
            wout_share.push()
        own_block(1)
        own_block(2)
        project(768, 1152)
        for h in range(HEADS):
            query, tan_query = head_pair(768, 0, h)
            queries[0:BLK, h * HD : (h + 1) * HD] = query
            queries[BLK:ROWS, h * HD : (h + 1) * HD] = tan_query
        if step == 0:
            while weight_ring.todo:
                weight_ring.advance(2)
                rings[0].advance(1)
            weight_ring.finish()

        spread = 15
        agenda = []
        for h in range(HEADS):
            size = 2 + 28
            for k in range(size - len(rings[h].todo), size):
                agenda.append((k + spread * h, 1, h, "advance"))
            if h:
                agenda.append((spread * h - 6, 0, h, "start"))
            agenda.append((size + spread * h, 2, h, "attend"))
        agenda.sort()

        def up(n):
            cols = slice(256 * n, 256 * (n + 1))
            pre = jnp.dot(x[...], wmlp[0, :, cols], preferred_element_type=F32)
            primal = jnp.concatenate([pre[0:HALF], pre[3 * HALF : ROWS]], axis=0)
            hidden, tan_hidden = gelu_pair(primal, pre[HALF : 3 * HALF])
            hidden = hidden.astype(BF16)
            hid[0:HALF, cols] = hidden[0:HALF]
            hid[HALF : 3 * HALF, cols] = tan_hidden.astype(BF16)
            hid[3 * HALF : ROWS, cols] = hidden[HALF:BLK]

        def down(i):
            units = feature_cols(lax.rem(tp + i, NTP))
            part[i % NTP] = lax.dot_general(
                hid[...], wmlp[1, units, :], (((1,), (1,)), ((), ())), preferred_element_type=F32
            ).astype(BF16)
            if i < NTP:
                copy = remote(
                    part.at[i, rows_sent],
                    got.at[i],
                    r_send.at[step, i],
                    r_recv.at[step, i],
                    tp_at(i),
                )
                copy.start()
                copies.append(copy)

        def collect_parts():
            total = part[0, rows_sent].astype(F32)
            for i in range(1, NTP):
                remote(
                    got.at[i], got.at[i], r_send.at[step, i], r_recv.at[step, i], tp_at(i)
                ).wait_recv()
                total = total + got[i].astype(F32)
            tot[rows_sent] = total
            piece = tot.at[half_rows(core)]
            copy = remote(piece, piece, p_send.at[step], p_recv.at[step], sibling())
            copy.start()
            copies.append(copy)

        first = pattern[0, 0]
        listed = [pattern[0, j] for j in range(K_SEL)]
        penalty = [
            jnp.where(listed[j] == first, NEG_BIG, 0.0).astype(F32) if j else None
            for j in range(K_SEL)
        ]
        scale = 1.0 / math.sqrt(HD)
        contract = (((1,), (1,)), ((), ()))

        def attend(h):
            kv, xa = kvs[h], xas[h]
            pair = queries[:, h * HD : (h + 1) * HD]
            scores, tan_scores = [], []
            for j in range(K_SEL):
                key, tan_key = kv[listed[j], 0], kv[listed[j], 1]
                both = lax.dot_general(pair, key, contract, preferred_element_type=F32) * scale
                cross = lax.dot_general(
                    pair[0:BLK], tan_key, contract, preferred_element_type=F32
                )
                score = both[0:BLK]
                scores.append(score + penalty[j] if j else score)
                tan_scores.append(both[BLK:ROWS] + cross * scale)
            top = scores[0]
            for j in range(1, K_SEL):
                top = jnp.maximum(top, scores[j])
            top = jnp.max(top, 1, keepdims=True)
            out = jnp.zeros((ROWS, 2 * HD), F32)
            weight_sum, tan_sum = jnp.zeros((BLK, BLK), F32), jnp.zeros((BLK, BLK), F32)
            for j in range(K_SEL):
                weights = jnp.exp(scores[j] - top)
                weighted = weights * tan_scores[j]
                weight_sum, tan_sum = weight_sum + weights, tan_sum + weighted
                left_side = jnp.concatenate([weights, weighted], axis=0).astype(BF16)
                values = jnp.concatenate([kv[listed[j], 3], kv[listed[j], 2]], axis=1)
                out = out + jnp.dot(left_side, values, preferred_element_type=F32)
            inv = 1.0 / jnp.sum(weight_sum, 1, keepdims=True)
            ratio = jnp.sum(tan_sum, 1, keepdims=True) * inv
            output = out[0:BLK, 0:HD] * inv
            tan_output = (out[0:BLK, HD : 2 * HD] + out[BLK:ROWS, 0:HD]) * inv - ratio * output
            output = output.astype(BF16)
            cols = head_cols(tp)
            xa[0:HALF, cols] = output[0:HALF]
            xa[HALF : 3 * HALF, cols] = tan_output.astype(BF16)
            xa[3 * HALF : ROWS, cols] = output[HALF:BLK]
            shares[h].push()

        def out_project(h):
            more = jnp.dot(
                xas[h][...], wo[h].reshape(NTP * HD, W), preferred_element_type=F32
            )
            acc[...] = more if h == 0 else acc[...] + more

        tasks = [partial(up, n) for n in range(3)] + [partial(down, i) for i in range(1, NTP + 1)]
        done = 0
        for _, _, h, what in agenda:
            if what == "start":
                rings[h].start()
            elif what == "advance":
                rings[h].advance(1)
                done += 1
                if tasks and done % 2 == 0:
                    tasks.pop(0)()
            else:
                rings[h].finish()
                while h == 0 and tasks:
                    tasks.pop(0)()
                attend(h)
                if h == 0 and step == 0:
                    wout_share.finish()
                if h == 1:
                    shares[0].finish()
                    out_project(0)
                    collect_parts()
        shares[1].finish()
        out_project(1)
        other = tot.at[half_rows(1 - core)]
        remote(other, other, p_send.at[step], p_recv.at[step], sibling()).wait_recv()
        shares[2].finish()
        out_project(2)
        branch = acc[...] + tot[...]
        gate = mod[3 * step + 2 : 3 * step + 3]
        change = change + jnp.sum(
            signs[...] * (gate * branch[HALF : 3 * HALF]), axis=1, keepdims=True
        )
        lat_out[0:HALF] += (1.0 / STEPS) * (gate * branch[0:HALF])
        lat_out[HALF:BLK] += (1.0 / STEPS) * (gate * branch[3 * HALF : ROWS])
        for copy in copies:
            copy.wait_send()
        for part_of in rings + shares + [x_share] + ([weight_ring, wout_share] if step == 0 else []):
            part_of.drain()

    copies = []
    dens[tp] = columns_to_rows([change])
    for i in range(1, NTP):
        copy = remote(dens.at[tp], dens.at[tp], d_send.at[i], d_recv.at[i], tp_at(i))
        copy.start()
        copies.append(copy)
    for i in range(1, NTP):
        there = dens.at[lax.rem(tp - i + NTP, NTP)]
        remote(there, there, d_send.at[i], d_recv.at[i], tp_at(i)).wait_recv()
    total = dens[0]
    for n in range(1, NTP):
        total = total + dens[n]
    dens[NTP] = total
    copy = remote(dens.at[NTP], dens.at[NTP + 1], d_send.at[0], d_recv.at[0], sibling())
    copy.start()
    remote(dens.at[NTP + 1], dens.at[NTP + 1], d_send.at[0], d_recv.at[0], sibling()).wait_recv()
    copies.append(copy)
    dens_out[...] = (dens[NTP] + dens[NTP + 1]) * (-1.0 / (STEPS * 2 * math.sqrt(full)))
    for copy in copies:
        copy.wait_send()


def local(latent, probes, modulation, pattern, w_qkv, w_out, w_up, w_down, q_gain, k_gain):
    start = lax.axis_index("tp") * W
    mod = lax.dynamic_slice_in_dim(modulation.reshape(3 * STEPS, D), start, W, 1)
    gains = jnp.stack([q_gain, k_gain])
    vmem, anywhere = pl.BlockSpec(memory_space=pltpu.VMEM), pl.BlockSpec(memory_space=pl.ANY)
    dma = pltpu.SemaphoreType.DMA
    latent_out, density = pl.pallas_call(
        body,
        out_shape=(
            jax.ShapeDtypeStruct((BLK, W), F32),
            jax.ShapeDtypeStruct((8, BLK), F32),
        ),
        in_specs=[vmem] * 4 + [pl.BlockSpec(memory_space=pltpu.SMEM)] + [anywhere] * 4,
        out_specs=(vmem, vmem),
        scratch_shapes=[pltpu.VMEM((NCTX, 4, BLK, HD), BF16) for _ in range(STEPS * HEADS)]
        + [
            pltpu.VMEM((D, 3 * W), BF16),
            pltpu.VMEM((HEADS, NTP, HD, W), BF16),
            pltpu.VMEM((2, D, UNITS), BF16),
            pltpu.VMEM((ROWS, D), BF16),
            pltpu.VMEM((ROWS, NTP * HD), BF16),
            pltpu.VMEM((ROWS, NTP * HD), BF16),
            pltpu.VMEM((ROWS, NTP * HD), BF16),
            pltpu.VMEM((BLK, W), F32),
            pltpu.VMEM((ROWS, 3 * W), F32),
            pltpu.VMEM((ROWS, W), BF16),
            pltpu.VMEM((ROWS, UNITS), BF16),
            pltpu.VMEM((ROWS, W), F32),
            pltpu.VMEM((NTP, ROWS, W), BF16),
            pltpu.VMEM((NTP, 3 * HALF, W), BF16),
            pltpu.VMEM((ROWS, W), F32),
            pltpu.VMEM((NTP, 8, BLK), F32),
            pltpu.VMEM((NTP + 2, 8, BLK), F32),
            dma((6,)),
        ]
        + [dma((STEPS, NTP)) for _ in range(4)]
        + [dma((STEPS,)) for _ in range(2)]
        + [dma((NTP,)) for _ in range(2)]
        + [dma((STEPS * HEADS + 1, 30)) for _ in range(4)]
        + [dma((STEPS * (HEADS + 1) + 1, NTP)) for _ in range(4)],
        compiler_params=pltpu.CompilerParams(
            collective_id=1, has_side_effects=True, vmem_limit_bytes=60 * 1024 * 1024
        ),
        name="euler_steps",
    )(
        latent,
        probes[0],
        mod,
        gains,
        pattern,
        w_qkv.transpose(1, 0, 2),
        w_out.reshape(HEADS, HD, D),
        w_up,
        w_down.T,
    )
    return latent_out, density[0]


def solution(mesh):
    return jax.shard_map(
        local,
        mesh=mesh,
        in_specs=(
            P("ctx", "tp"),
            P("probe", "ctx", "tp"),
            P(),
            P("ctx", None),
            P(None, None, "tp"),
            P("tp", None),
            P("ctx", "tp"),
            P("tp", "ctx"),
            P("tp"),
            P("tp"),
        ),
        out_specs=(P("ctx", "tp"), P("ctx")),
        check_vma=False,
    )
```

```python
from functools import partial
import math

import jax
import jax.numpy as jnp
from jax import lax
from jax.experimental import pallas as pl
from jax.experimental.pallas import tpu as pltpu
from jax.sharding import PartitionSpec as P

HD = 128
BLK = 128
K_SEL = 8
STEPS = 2
NTP = 8
NZ = 8
NCTX = 16
W = 384
D = 3072
HEADS = 3
GROUPS = ((0, 1), (2,))
NG = len(GROUPS)
UNITS = 768
SHARD = 192
HALF = 64
ROWS = 256

EPS = 1e-06
NEG_BIG = -1e30
MESH = pl.DeviceIdType.MESH
F32 = jnp.float32
BF16 = jnp.bfloat16


def place():
    return lax.axis_index("ctx"), lax.axis_index("tp"), lax.axis_index("probe")


def tp_at(offset):
    ctx, tp, core = place()
    return (ctx, lax.rem(tp + offset + NTP, NTP), core)


def tp_of(x, y):
    ctx, _, core = place()
    return (ctx, lax.rem(x, 4) * 2 + y, core)


def sibling():
    ctx, tp, core = place()
    return (ctx, tp, 1 - core)


def ctx_at(block):
    _, tp, core = place()
    return (block, tp, core)


def ring_devices():
    ctx, _, _ = place()
    z, h = lax.rem(ctx, NZ), lax.div(ctx, NZ)
    right = h * NZ + lax.rem(z + 1, NZ)
    left = h * NZ + lax.rem(z + NZ - 1, NZ)
    across = (1 - h) * NZ + z
    return ctx_at(right), ctx_at(left), ctx_at(across)


def greet(devices):
    barrier = pltpu.get_barrier_semaphore()
    for device in devices:
        pl.semaphore_signal(barrier, inc=1, device_id=device, device_id_type=MESH)
    pl.semaphore_wait(barrier, len(devices))


def remote(src, dst, send_sem, recv_sem, device):
    return pltpu.make_async_remote_copy(
        src_ref=src,
        dst_ref=dst,
        send_sem=send_sem,
        recv_sem=recv_sem,
        device_id=device,
        device_id_type=MESH,
    )


def feature_cols(owner):
    return pl.ds(pl.multiple_of(owner * W, 128), W)


def group_cols(owner, size):
    return pl.ds(pl.multiple_of(owner * size * HD, 128), size * HD)


def half_rows(core):
    return pl.ds(pl.multiple_of(core * 3 * HALF, HALF), HALF)


class Ring:
    def __init__(self, own, passed, given, sems):
        self.own, self.passed, self.given = own, passed, given
        self.send, self.recv, self.f_send, self.f_recv = sems
        ctx, _, core = place()
        z, h = lax.rem(ctx, NZ), lax.div(ctx, NZ)
        self.ctx = ctx
        right, left, across = ring_devices()
        turn = 1 - 2 * core
        ahead = ctx_at(h * NZ + lax.rem(z + turn + NZ, NZ))
        behind = ctx_at(h * NZ + lax.rem(z - turn + NZ, NZ))
        self.right, self.left, self.across, self.ahead, self.behind = right, left, across, ahead, behind
        self.copies, self.taken = [], []

        def at(row, step):
            return row * NZ + lax.rem(z + step + NZ, NZ)

        self.todo = [
            (at(1 - h, 0), 0, 0, ((5, right), (11, left))),
            (at(1 - h, 0), 1, 22, ()),
        ]
        for s in range(1, 5):
            for row, step, base, reach, device in (
                (h, -s, 0, 4, right),
                (h, s, 7, 3, left),
            ):
                if s <= reach:
                    onward = ((base + s + 1, device),) if s < reach else ()
                    self.todo.append((at(row, step), 0, base + s, onward))
            for step, base, y_base, reach, device in (
                (-s * turn, 14, 22, 4, ahead),
                (s * turn, 18, 26, 3, behind),
            ):
                if s <= reach:
                    onward = ((base + s + 1, device),) if s < reach else ()
                    onward = onward + ((y_base + s, across),)
                    self.todo.append((at(h, step), 1, base + s, onward))
            for row, step, base, reach, device in (
                (1 - h, -s, 4, 3, right),
                (1 - h, s, 10, 4, left),
            ):
                if s <= reach:
                    onward = ((base + s + 1, device),) if s < reach else ()
                    self.todo.append((at(row, step), 0, base + s, onward))
            self.todo.append((at(1 - h, -s * turn), 1, 22 + s, ()))
            if s <= 3:
                self.todo.append((at(1 - h, s * turn), 1, 26 + s, ()))

    def push(self, block, part, n, device):
        piece = self.own(block, part)
        copy = remote(piece, piece, self.send.at[n], self.recv.at[n], device)
        copy.start()
        self.copies.append(copy)

    def start(self):
        self.push(self.ctx, 0, 0, self.across)
        self.push(self.ctx, 0, 1, self.right)
        self.push(self.ctx, 0, 8, self.left)
        self.push(self.ctx, 1, 15, self.ahead)
        self.push(self.ctx, 1, 19, self.behind)
        self.push(self.ctx, 1, 22, self.across)

    def advance(self, count=1):
        for _ in range(count):
            if not self.todo:
                return
            block, part, n, onward = self.todo.pop(0)
            mine = self.own(block, part)
            remote(mine, mine, self.send.at[n], self.recv.at[n], self.across).wait_recv()
            for later, device in onward:
                self.push(block, part, later, device)
            piece = self.passed(block, part)
            copy = remote(piece, piece, self.f_send.at[n], self.f_recv.at[n], sibling())
            copy.start()
            self.copies.append(copy)
            self.taken.append((block, part, n))

    def finish(self):
        self.advance(len(self.todo))
        for block, part, n in self.taken:
            piece = self.given(block, part)
            remote(piece, piece, self.f_send.at[n], self.f_recv.at[n], sibling()).wait_recv()

    def drain(self):
        for copy in self.copies:
            copy.wait_send()


class Share:
    def __init__(self, piece, passed, given, sems):
        self.piece, self.passed, self.given = piece, passed, given
        self.send, self.recv, self.f_send, self.f_recv = sems
        self.tp = lax.axis_index("tp")
        self.copies, self.taken = [], []
        x, y = lax.div(self.tp, 2), lax.rem(self.tp, 2)
        self.beside = tp_of(x, 1 - y)
        self.along = [tp_of(x + d, y) for d in range(4)]

        def at(dx, row):
            return lax.rem(x + dx, 4) * 2 + row

        relay = tuple((3 + d, self.along[d]) for d in (2, 1, 3))
        self.todo = [(at(0, 1 - y), 0, relay)]
        for row, base in ((y, 0), (1 - y, 3)):
            self.todo += [(at(4 - d, row), base + d, ()) for d in (1, 3, 2)]

    def start(self, owner, n, device):
        here = self.piece(owner)
        copy = remote(here, here, self.send.at[n], self.recv.at[n], device)
        copy.start()
        self.copies.append(copy)

    def push(self):
        self.start(self.tp, 0, self.beside)
        for d in (2, 1, 3):
            self.start(self.tp, d, self.along[d])

    def collect(self, count=NTP):
        while self.todo and count:
            owner, n, onward = self.todo.pop(0)
            here = self.piece(owner)
            remote(here, here, self.send.at[n], self.recv.at[n], self.beside).wait_recv()
            for later, device in onward:
                self.start(owner, later, device)
            count -= 1
            if self.passed is None:
                continue
            part = self.passed(owner)
            copy = remote(part, part, self.f_send.at[n], self.f_recv.at[n], sibling())
            copy.start()
            self.copies.append(copy)
            self.taken.append((owner, n))

    def finish(self):
        self.collect()
        for owner, n in self.taken:
            part = self.given(owner)
            remote(part, part, self.f_send.at[n], self.f_recv.at[n], sibling()).wait_recv()

    def drain(self):
        for copy in self.copies:
            copy.wait_send()


class Exchange(Share):
    def __init__(self, piece, passed, given, sems, source=None):
        super().__init__(piece, passed, given, sems)
        self.source = source or (lambda i: piece(self.tp))
        self.todo = [(lax.rem(self.tp - i + NTP, NTP), i, ()) for i in range(1, NTP)]

    def push(self):
        for i in range(1, NTP):
            copy = remote(
                self.source(i), self.piece(self.tp), self.send.at[i], self.recv.at[i], tp_at(i)
            )
            copy.start()
            self.copies.append(copy)


def gelu_pair(pre, tan_pre):
    c = math.sqrt(2.0 / math.pi)
    square = pre * pre
    t = jnp.tanh(c * (pre + 0.044715 * (square * pre)))
    half = 0.5 * (1.0 + t)
    slope = half + 0.5 * pre * (1.0 - t * t) * (c * (1.0 + 3.0 * 0.044715 * square))
    return pre * half, slope * tan_pre


def columns_to_rows(columns):
    lane = lax.broadcasted_iota(jnp.int32, (BLK, BLK), 1)
    packed = jnp.zeros((BLK, BLK), F32)
    for n, column in enumerate(columns):
        packed = jnp.where(lane == n, column, packed)
    return packed.T[0:8]


def rows_to_columns(rows):
    return jnp.concatenate([rows, jnp.zeros((BLK - 8, BLK), F32)], axis=0).T


def body(
    lat, probes, mod, gains, pattern, wqkv_hbm, wout_hbm, wup_hbm, wdn_hbm,
    lat_out, dens_out,
    kv_0, kv_1, kv_2, kv_3,
    wqkv, wo, wmlp, x, xa_0, xa_1, sg, signs, proj, queries, hid, acc, part, got, cross, tot, stat, dens,
    w_sem, s_send, s_recv, r_send, r_recv, p_send, p_recv, d_send, d_recv,
    *many_sems,
):
    ring_sems, share_sems = many_sems[:4], many_sems[4:]
    ctx, tp, core = place()
    column, y = lax.div(tp, 2), lax.rem(tp, 2)
    mine = feature_cols(tp)
    rows_sent = pl.ds(pl.multiple_of(core * HALF, HALF), 3 * HALF)
    my_half = pl.ds(pl.multiple_of(core * (W // 2), HALF), W // 2)
    other_half = pl.ds(pl.multiple_of((1 - core) * (W // 2), HALF), W // 2)
    full = float(D)
    shard = pl.ds(pl.multiple_of(ctx * SHARD, 64), SHARD)
    loads = [
        pltpu.make_async_copy(wup_hbm, wmlp.at[0, shard], w_sem.at[0]),
        pltpu.make_async_copy(wdn_hbm, wmlp.at[1, shard], w_sem.at[1]),
        pltpu.make_async_copy(wqkv_hbm.at[1], wqkv.at[:, 0:W], w_sem.at[2]),
        pltpu.make_async_copy(wqkv_hbm.at[2], wqkv.at[:, W : 2 * W], w_sem.at[3]),
        pltpu.make_async_copy(wqkv_hbm.at[0], wqkv.at[:, 2 * W : 3 * W], w_sem.at[4]),
        pltpu.make_async_copy(wout_hbm.at[:, mine], wo.at[tp], w_sem.at[5]),
    ]
    for load in loads:
        load.start()
    signs[...] = 2.0 * probes[...].astype(F32) - 1.0
    lat_out[...] = lat[...]
    right, left, across = ring_devices()
    greet([tp_at(i) for i in range(1, NTP)] + [right, left, across, sibling()])

    def block_rows(block, part):
        start = block * SHARD + part * (SHARD - HALF)
        return pl.ds(pl.multiple_of(start, HALF), HALF if part else SHARD - HALF)

    weight_ring = Ring(
        lambda block, part: wmlp.at[core, block_rows(block, part)],
        lambda block, part: wmlp.at[core, block_rows(block, part)],
        lambda block, part: wmlp.at[1 - core, block_rows(block, part)],
        [sems.at[STEPS * NG] for sems in ring_sems],
    )
    wout_share = Exchange(
        lambda owner: wo.at[owner, my_half],
        lambda owner: wo.at[owner, my_half],
        lambda owner: wo.at[owner, other_half],
        [sems.at[STEPS * (NG + 1)] for sems in share_sems],
        lambda i: wout_hbm.at[my_half, feature_cols(lax.rem(tp + i, NTP))],
    )
    sg[:, mine] = signs[...].astype(BF16)
    sign_share = Exchange(
        lambda owner: sg.at[:, feature_cols(owner)],
        None,
        None,
        [sems.at[STEPS * (NG + 1) + 1] for sems in share_sems],
    )
    sign_share.push()
    loads[0].wait()
    loads[1].wait()
    weight_ring.start()
    change = jnp.zeros((BLK, 1), F32)

    for step in range(STEPS):
        copies = []
        kvs = (kv_0, kv_1, kv_2, kv_3)[NG * step : NG * (step + 1)]
        xas = (xa_0, xa_1)
        rows, tangent = lat_out[...], signs[...]
        stat[tp] = columns_to_rows(
            [
                jnp.sum(rows, 1, keepdims=True),
                jnp.sum(rows * rows, 1, keepdims=True),
                jnp.sum(tangent, 1, keepdims=True),
                jnp.sum(rows * tangent, 1, keepdims=True),
            ]
        )
        for i in range(1, NTP):
            copy = remote(
                stat.at[tp], stat.at[tp], s_send.at[step, i], s_recv.at[step, i], tp_at(i)
            )
            copy.start()
            copies.append(copy)
        for i in range(1, NTP):
            there = stat.at[lax.rem(tp - i + NTP, NTP)]
            remote(there, there, s_send.at[step, i], s_recv.at[step, i], tp_at(i)).wait_recv()
        total = stat[0]
        for n in range(1, NTP):
            total = total + stat[n]
        total = rows_to_columns(total) * (1.0 / full)
        row_mean, row_sq, tan_mean, tan_sq = (total[:, n : n + 1] for n in range(4))
        row_var = row_sq - row_mean * row_mean
        tan_var = 2.0 * (tan_sq - row_mean * tan_mean)
        inv_std = lax.rsqrt(row_var + EPS)
        centred = rows - row_mean
        shift, gain = mod[3 * step : 3 * step + 1, mine], 1.0 + mod[3 * step + 1 : 3 * step + 2, mine]
        normed = (centred * inv_std * gain + shift).astype(BF16)
        x[0:HALF, mine] = normed[0:HALF]
        x[3 * HALF : ROWS, mine] = normed[HALF:BLK]
        x_share = Exchange(
            lambda owner: x.at[half_rows(core), feature_cols(owner)],
            lambda owner: x.at[half_rows(core), feature_cols(owner)],
            lambda owner: x.at[half_rows(1 - core), feature_cols(owner)],
            [sems.at[step] for sems in share_sems],
        )
        x_share.push()
        if step == 0:
            weight_ring.advance(2)
            sign_share.finish()
            weight_ring.advance(2)
            x_share.collect(4)
            weight_ring.advance(2)
        x_share.finish()
        inv_rows = jnp.broadcast_to(inv_std, (BLK, W))
        mean_rows = jnp.broadcast_to(inv_std * tan_mean, (BLK, W))
        var_rows = jnp.broadcast_to(0.5 * inv_std * inv_std * tan_var, (BLK, W))
        for n in range(NTP):
            cols = slice(n * W, (n + 1) * W)
            primal = jnp.concatenate([x[0:HALF, cols], x[3 * HALF : ROWS, cols]], axis=0)
            scaled = primal.astype(F32) - mod[3 * step : 3 * step + 1, cols]
            turned = (inv_rows * sg[:, cols].astype(F32) - mean_rows) * (
                1.0 + mod[3 * step + 1 : 3 * step + 2, cols]
            )
            x[HALF : 3 * HALF, cols] = (turned - var_rows * scaled).astype(BF16)
        if step == 0:
            for load in loads[2:]:
                load.wait()

        def head_pair(column, gain_row, h):
            view = proj[:, column + h * HD : column + (h + 1) * HD]
            primal = jnp.concatenate([view[0:HALF], view[3 * HALF : ROWS]], axis=0)
            tan = view[HALF : 3 * HALF]
            gain_view = gains[gain_row : gain_row + 1, h * HD : (h + 1) * HD]
            inv = lax.rsqrt(jnp.mean(primal * primal, 1, keepdims=True) + EPS)
            tan_inv = -inv * inv * inv * jnp.mean(primal * tan, 1, keepdims=True)
            return (
                (primal * inv * gain_view).astype(BF16),
                ((tan * inv + primal * tan_inv) * gain_view).astype(BF16),
            )

        def project(start, stop):
            proj[:, start:stop] = jnp.dot(
                x[...], wqkv[:, start:stop], preferred_element_type=F32
            )

        def own_block(g):
            kv = kvs[g]
            for n, h in enumerate(GROUPS[g]):
                key, tan_key = head_pair(0, 1, h)
                cols, to = slice(W + h * HD, W + (h + 1) * HD), slice(n * HD, (n + 1) * HD)
                kv[ctx, 0, :, to] = key
                kv[ctx, 1, :, to] = tan_key
                kv[ctx, 2, :, to] = proj[HALF : 3 * HALF, cols].astype(BF16)
                kv[ctx, 3, 0:HALF, to] = proj[0:HALF, cols].astype(BF16)
                kv[ctx, 3, HALF:BLK, to] = proj[3 * HALF : ROWS, cols].astype(BF16)

        def part_rows(part):
            return slice(part * HALF, (part + 1) * HALF)

        rings = [
            Ring(
                lambda block, part, kv=kv: kv.at[block, pl.ds(core, 3), part_rows(part)],
                lambda block, part, kv=kv: kv.at[block, pl.ds(core * 3, 1), part_rows(part)],
                lambda block, part, kv=kv: kv.at[block, pl.ds((1 - core) * 3, 1), part_rows(part)],
                [sems.at[step * NG + g] for sems in ring_sems],
            )
            for g, kv in enumerate(kvs)
        ]
        shares = [
            (Share, Exchange)[g](
                lambda owner, xa=xa, g=g: xa.at[rows_sent, group_cols(owner, len(GROUPS[g]))],
                lambda owner, xa=xa, g=g: xa.at[half_rows(core), group_cols(owner, len(GROUPS[g]))],
                lambda owner, xa=xa, g=g: xa.at[
                    half_rows(1 - core), group_cols(owner, len(GROUPS[g]))
                ],
                [sems.at[STEPS + step * NG + g] for sems in share_sems],
            )
            for g, xa in enumerate(xas)
        ]
        for n in range(3):
            project(256 * n, 256 * (n + 1))
        own_block(0)
        rings[0].start()
        if step == 0:
            weight_ring.advance(4)
            wout_share.push()
        own_block(1)
        project(768, 1152)
        for h in range(HEADS):
            query, tan_query = head_pair(768, 0, h)
            queries[0:BLK, h * HD : (h + 1) * HD] = query
            queries[BLK:ROWS, h * HD : (h + 1) * HD] = tan_query
        if step == 0:
            while weight_ring.todo:
                weight_ring.advance(2)
                rings[0].advance(1)
            weight_ring.finish()

        def up(n):
            cols = slice(256 * n, 256 * (n + 1))
            pre = jnp.dot(x[...], wmlp[0, :, cols], preferred_element_type=F32)
            primal = jnp.concatenate([pre[0:HALF], pre[3 * HALF : ROWS]], axis=0)
            hidden, tan_hidden = gelu_pair(primal, pre[HALF : 3 * HALF])
            hidden = hidden.astype(BF16)
            hid[0:HALF, cols] = hidden[0:HALF]
            hid[HALF : 3 * HALF, cols] = tan_hidden.astype(BF16)
            hid[3 * HALF : ROWS, cols] = hidden[HALF:BLK]

        def down(d, k):
            row = y if k == 0 else 1 - y
            units = feature_cols(lax.rem(column + d, 4) * 2 + row)
            part[d, k] = lax.dot_general(
                hid[...], wmlp[1, units, :], (((1,), (1,)), ((), ())), preferred_element_type=F32
            ).astype(BF16)
            if d and k:
                copy = remote(
                    part.at[d, :, rows_sent],
                    got.at[d - 1],
                    r_send.at[step, d],
                    r_recv.at[step, d],
                    tp_of(column + d, y),
                )
                copy.start()
                copies.append(copy)

        def collect_column():
            for d in range(1, 4):
                remote(
                    got.at[d - 1], got.at[d - 1], r_send.at[step, d], r_recv.at[step, d], sibling()
                ).wait_recv()
            total = part[0, 1, rows_sent].astype(F32)
            for d in range(3):
                total = total + got[d, 1].astype(F32)
            cross[0] = total.astype(BF16)
            copy = remote(
                cross.at[0],
                cross.at[1],
                r_send.at[step, 0],
                r_recv.at[step, 0],
                tp_of(column, 1 - y),
            )
            copy.start()
            copies.append(copy)

        def collect_parts():
            total = part[0, 0, rows_sent].astype(F32)
            for d in range(3):
                total = total + got[d, 0].astype(F32)
            remote(
                cross.at[1], cross.at[1], r_send.at[step, 0], r_recv.at[step, 0], sibling()
            ).wait_recv()
            tot[rows_sent] = total + cross[1].astype(F32)
            piece = tot.at[half_rows(core)]
            copy = remote(piece, piece, p_send.at[step], p_recv.at[step], sibling())
            copy.start()
            copies.append(copy)

        first = pattern[0, 0]
        listed = [pattern[0, j] for j in range(K_SEL)]
        penalty = [
            jnp.where(listed[j] == first, NEG_BIG, 0.0).astype(F32) if j else None
            for j in range(K_SEL)
        ]
        scale = 1.0 / math.sqrt(HD)
        contract = (((1,), (1,)), ((), ()))

        def attend(g, n):
            kv, xa, h = kvs[g], xas[g], GROUPS[g][n]
            own = slice(n * HD, (n + 1) * HD)
            pair = queries[:, h * HD : (h + 1) * HD]
            scores, tan_scores = [], []
            for j in range(K_SEL):
                key, tan_key = kv[listed[j], 0, :, own], kv[listed[j], 1, :, own]
                both = lax.dot_general(pair, key, contract, preferred_element_type=F32) * scale
                crossed = lax.dot_general(
                    pair[0:BLK], tan_key, contract, preferred_element_type=F32
                )
                score = both[0:BLK]
                scores.append(score + penalty[j] if j else score)
                tan_scores.append(both[BLK:ROWS] + crossed * scale)
            top = scores[0]
            for j in range(1, K_SEL):
                top = jnp.maximum(top, scores[j])
            top = jnp.max(top, 1, keepdims=True)
            out = jnp.zeros((ROWS, 2 * HD), F32)
            weight_sum, tan_sum = jnp.zeros((BLK, BLK), F32), jnp.zeros((BLK, BLK), F32)
            for j in range(K_SEL):
                weights = jnp.exp(scores[j] - top)
                weighted = weights * tan_scores[j]
                weight_sum, tan_sum = weight_sum + weights, tan_sum + weighted
                left_side = jnp.concatenate([weights, weighted], axis=0).astype(BF16)
                values = jnp.concatenate(
                    [kv[listed[j], 3, :, own], kv[listed[j], 2, :, own]], axis=1
                )
                out = out + jnp.dot(left_side, values, preferred_element_type=F32)
            inv = 1.0 / jnp.sum(weight_sum, 1, keepdims=True)
            ratio = jnp.sum(tan_sum, 1, keepdims=True) * inv
            output = out[0:BLK, 0:HD] * inv
            tan_output = (out[0:BLK, HD : 2 * HD] + out[BLK:ROWS, 0:HD]) * inv - ratio * output
            output = output.astype(BF16)
            cols = pl.ds(pl.multiple_of((tp * len(GROUPS[g]) + n) * HD, 128), HD)
            xa[0:HALF, cols] = output[0:HALF]
            xa[HALF : 3 * HALF, cols] = tan_output.astype(BF16)
            xa[3 * HALF : ROWS, cols] = output[HALF:BLK]

        def out_project(g):
            size = len(GROUPS[g]) * HD
            rows = wo[:, GROUPS[g][0] * HD : GROUPS[g][0] * HD + size].reshape(NTP * size, W)
            more = jnp.dot(xas[g][...], rows, preferred_element_type=F32)
            acc[...] = more if g == 0 else acc[...] + more

        tasks = [partial(up, n) for n in range(3)] + [
            partial(down, d, k) for d in (2, 1, 3, 0) for k in (0, 1)
        ]
        had = 30 - len(rings[0].todo)
        agenda = [(k, 1, rings[0].advance) for k in range(had, 30)]
        agenda += [(max(9, had), 0, rings[1].start)]
        agenda += [(15 + k, 2, rings[1].advance) for k in range(30)]
        agenda += [(had + 1 + n * (1.6 if step else 1.1), 3, task) for n, task in enumerate(tasks)]
        agenda += [
            (30, 4, rings[0].finish),
            (30, 5, partial(attend, 0, 0)),
            (33, 5, partial(attend, 0, 1)),
            (33, 6, shares[0].push),
            (36, 5, collect_column),
            (38, 5, partial(shares[0].collect, 1)),
            (45, 5, rings[1].finish),
            (45, 6, partial(attend, 1, 0)),
            (45, 7, shares[1].push),
            (46, 0, shares[0].finish),
            (46, 1, collect_parts),
        ]
        if step == 0:
            agenda.append((35, 5, wout_share.finish))
        for _, _, task in sorted(agenda, key=lambda entry: entry[:2]):
            task()
        out_project(0)
        other = tot.at[half_rows(1 - core)]
        remote(other, other, p_send.at[step], p_recv.at[step], sibling()).wait_recv()
        shares[1].finish()
        out_project(1)
        branch = acc[...] + tot[...]
        gate = mod[3 * step + 2 : 3 * step + 3, mine]
        change = change + jnp.sum(
            signs[...] * (gate * branch[HALF : 3 * HALF]), axis=1, keepdims=True
        )
        lat_out[0:HALF] += (1.0 / STEPS) * (gate * branch[0:HALF])
        lat_out[HALF:BLK] += (1.0 / STEPS) * (gate * branch[3 * HALF : ROWS])
        for copy in copies:
            copy.wait_send()
        for part_of in rings + shares + [x_share] + ([weight_ring, wout_share, sign_share] if step == 0 else []):
            part_of.drain()

    copies = []
    dens[tp] = columns_to_rows([change])
    for i in range(1, NTP):
        copy = remote(dens.at[tp], dens.at[tp], d_send.at[i], d_recv.at[i], tp_at(i))
        copy.start()
        copies.append(copy)
    for i in range(1, NTP):
        there = dens.at[lax.rem(tp - i + NTP, NTP)]
        remote(there, there, d_send.at[i], d_recv.at[i], tp_at(i)).wait_recv()
    total = dens[0]
    for n in range(1, NTP):
        total = total + dens[n]
    dens[NTP] = total
    copy = remote(dens.at[NTP], dens.at[NTP + 1], d_send.at[0], d_recv.at[0], sibling())
    copy.start()
    remote(dens.at[NTP + 1], dens.at[NTP + 1], d_send.at[0], d_recv.at[0], sibling()).wait_recv()
    copies.append(copy)
    dens_out[...] = (dens[NTP] + dens[NTP + 1]) * (-1.0 / (STEPS * 2 * math.sqrt(full)))
    for copy in copies:
        copy.wait_send()


def local(latent, probes, modulation, pattern, w_qkv, w_out, w_up, w_down, q_gain, k_gain):
    mod = modulation.reshape(3 * STEPS, D)
    gains = jnp.stack([q_gain, k_gain])
    vmem, anywhere = pl.BlockSpec(memory_space=pltpu.VMEM), pl.BlockSpec(memory_space=pl.ANY)
    dma = pltpu.SemaphoreType.DMA
    latent_out, density = pl.pallas_call(
        body,
        out_shape=(
            jax.ShapeDtypeStruct((BLK, W), F32),
            jax.ShapeDtypeStruct((8, BLK), F32),
        ),
        in_specs=[vmem] * 4 + [pl.BlockSpec(memory_space=pltpu.SMEM)] + [anywhere] * 4,
        out_specs=(vmem, vmem),
        scratch_shapes=[
            pltpu.VMEM((NCTX, 4, BLK, len(group) * HD), BF16)
            for _ in range(STEPS)
            for group in GROUPS
        ]
        + [
            pltpu.VMEM((D, 3 * W), BF16),
            pltpu.VMEM((NTP, W, W), BF16),
            pltpu.VMEM((2, D, UNITS), BF16),
            pltpu.VMEM((ROWS, D), BF16),
            pltpu.VMEM((ROWS, NTP * len(GROUPS[0]) * HD), BF16),
            pltpu.VMEM((ROWS, NTP * len(GROUPS[1]) * HD), BF16),
            pltpu.VMEM((BLK, D), BF16),
            pltpu.VMEM((BLK, W), F32),
            pltpu.VMEM((ROWS, 3 * W), F32),
            pltpu.VMEM((ROWS, W), BF16),
            pltpu.VMEM((ROWS, UNITS), BF16),
            pltpu.VMEM((ROWS, W), F32),
            pltpu.VMEM((4, 2, ROWS, W), BF16),
            pltpu.VMEM((3, 2, 3 * HALF, W), BF16),
            pltpu.VMEM((2, 3 * HALF, W), BF16),
            pltpu.VMEM((ROWS, W), F32),
            pltpu.VMEM((NTP, 8, BLK), F32),
            pltpu.VMEM((NTP + 2, 8, BLK), F32),
            dma((6,)),
        ]
        + [dma((STEPS, NTP)) for _ in range(4)]
        + [dma((STEPS,)) for _ in range(2)]
        + [dma((NTP,)) for _ in range(2)]
        + [dma((STEPS * NG + 1, 30)) for _ in range(4)]
        + [dma((STEPS * (NG + 1) + 2, NTP)) for _ in range(4)],
        compiler_params=pltpu.CompilerParams(
            collective_id=1, has_side_effects=True, vmem_limit_bytes=60 * 1024 * 1024
        ),
        name="euler_steps",
    )(
        latent,
        probes[0],
        mod,
        gains,
        pattern,
        w_qkv.transpose(1, 0, 2),
        w_out,
        w_up,
        w_down.T,
    )
    return latent_out, density[0]


def solution(mesh):
    return jax.shard_map(
        local,
        mesh=mesh,
        in_specs=(
            P("ctx", "tp"),
            P("probe", "ctx", "tp"),
            P(),
            P("ctx", None),
            P(None, None, "tp"),
            P("tp", None),
            P("ctx", "tp"),
            P("tp", "ctx"),
            P("tp"),
            P("tp"),
        ),
        out_specs=(P("ctx", "tp"), P("ctx")),
        check_vma=False,
    )
```

```python
from functools import partial
import math

import jax
import jax.numpy as jnp
from jax import lax
from jax.experimental import pallas as pl
from jax.experimental.pallas import tpu as pltpu
from jax.sharding import PartitionSpec as P

HD = 128
BLK = 128
K_SEL = 8
STEPS = 2
NTP = 8
NZ = 8
NCTX = 16
W = 384
D = 3072
HEADS = 3
GROUPS = ((0, 1), (2,))
NG = len(GROUPS)
UNITS = 768
SHARD = 192
HALF = 64
ROWS = 256

EPS = 1e-06
NEG_BIG = -1e30
MESH = pl.DeviceIdType.MESH
F32 = jnp.float32
BF16 = jnp.bfloat16


def place():
    return lax.axis_index("ctx"), lax.axis_index("tp"), lax.axis_index("probe")


def tp_at(offset):
    ctx, tp, core = place()
    return (ctx, lax.rem(tp + offset + NTP, NTP), core)


def tp_of(x, y):
    ctx, _, core = place()
    return (ctx, lax.rem(x, 4) * 2 + y, core)


def sibling():
    ctx, tp, core = place()
    return (ctx, tp, 1 - core)


def ctx_at(block):
    _, tp, core = place()
    return (block, tp, core)


def ring_devices():
    ctx, _, _ = place()
    z, h = lax.rem(ctx, NZ), lax.div(ctx, NZ)
    right = h * NZ + lax.rem(z + 1, NZ)
    left = h * NZ + lax.rem(z + NZ - 1, NZ)
    across = (1 - h) * NZ + z
    return ctx_at(right), ctx_at(left), ctx_at(across)


def greet(devices):
    barrier = pltpu.get_barrier_semaphore()
    for device in devices:
        pl.semaphore_signal(barrier, inc=1, device_id=device, device_id_type=MESH)
    pl.semaphore_wait(barrier, len(devices))


def remote(src, dst, send_sem, recv_sem, device):
    return pltpu.make_async_remote_copy(
        src_ref=src,
        dst_ref=dst,
        send_sem=send_sem,
        recv_sem=recv_sem,
        device_id=device,
        device_id_type=MESH,
    )


def feature_cols(owner):
    return pl.ds(pl.multiple_of(owner * W, 128), W)


def group_cols(owner, size):
    return pl.ds(pl.multiple_of(owner * size * HD, 128), size * HD)


def half_rows(core):
    return pl.ds(pl.multiple_of(core * 3 * HALF, HALF), HALF)


class Ring:
    def __init__(self, own, passed, given, sems):
        self.own, self.passed, self.given = own, passed, given
        self.send, self.recv, self.f_send, self.f_recv = sems
        ctx, _, core = place()
        z, h = lax.rem(ctx, NZ), lax.div(ctx, NZ)
        self.ctx = ctx
        right, left, across = ring_devices()
        turn = 1 - 2 * core
        ahead = ctx_at(h * NZ + lax.rem(z + turn + NZ, NZ))
        behind = ctx_at(h * NZ + lax.rem(z - turn + NZ, NZ))
        self.right, self.left, self.across, self.ahead, self.behind = right, left, across, ahead, behind
        self.copies, self.taken = [], []

        def at(row, step):
            return row * NZ + lax.rem(z + step + NZ, NZ)

        self.todo = [
            (at(1 - h, 0), 0, 0, ((5, right), (11, left))),
            (at(1 - h, 0), 1, 22, ()),
        ]
        for s in range(1, 5):
            for row, step, base, reach, device in (
                (h, -s, 0, 4, right),
                (h, s, 7, 3, left),
            ):
                if s <= reach:
                    onward = ((base + s + 1, device),) if s < reach else ()
                    self.todo.append((at(row, step), 0, base + s, onward))
            for step, base, y_base, reach, device in (
                (-s * turn, 14, 22, 4, ahead),
                (s * turn, 18, 26, 3, behind),
            ):
                if s <= reach:
                    onward = ((base + s + 1, device),) if s < reach else ()
                    onward = onward + ((y_base + s, across),)
                    self.todo.append((at(h, step), 1, base + s, onward))
            for row, step, base, reach, device in (
                (1 - h, -s, 4, 3, right),
                (1 - h, s, 10, 4, left),
            ):
                if s <= reach:
                    onward = ((base + s + 1, device),) if s < reach else ()
                    self.todo.append((at(row, step), 0, base + s, onward))
            self.todo.append((at(1 - h, -s * turn), 1, 22 + s, ()))
            if s <= 3:
                self.todo.append((at(1 - h, s * turn), 1, 26 + s, ()))

    def push(self, block, part, n, device):
        piece = self.own(block, part)
        copy = remote(piece, piece, self.send.at[n], self.recv.at[n], device)
        copy.start()
        self.copies.append(copy)

    def start(self):
        self.push(self.ctx, 0, 0, self.across)
        self.push(self.ctx, 0, 1, self.right)
        self.push(self.ctx, 0, 8, self.left)
        self.push(self.ctx, 1, 15, self.ahead)
        self.push(self.ctx, 1, 19, self.behind)
        self.push(self.ctx, 1, 22, self.across)

    def advance(self, count=1):
        for _ in range(count):
            if not self.todo:
                return
            block, part, n, onward = self.todo.pop(0)
            mine = self.own(block, part)
            remote(mine, mine, self.send.at[n], self.recv.at[n], self.across).wait_recv()
            for later, device in onward:
                self.push(block, part, later, device)
            piece = self.passed(block, part)
            copy = remote(piece, piece, self.f_send.at[n], self.f_recv.at[n], sibling())
            copy.start()
            self.copies.append(copy)
            self.taken.append((block, part, n))

    def finish(self):
        self.advance(len(self.todo))
        for block, part, n in self.taken:
            piece = self.given(block, part)
            remote(piece, piece, self.f_send.at[n], self.f_recv.at[n], sibling()).wait_recv()

    def drain(self):
        for copy in self.copies:
            copy.wait_send()


class Share:
    def __init__(self, piece, passed, given, sems):
        self.piece, self.passed, self.given = piece, passed, given
        self.send, self.recv, self.f_send, self.f_recv = sems
        self.tp = lax.axis_index("tp")
        self.copies, self.taken = [], []
        x, y = lax.div(self.tp, 2), lax.rem(self.tp, 2)
        self.beside = tp_of(x, 1 - y)
        self.along = [tp_of(x + d, y) for d in range(4)]

        def at(dx, row):
            return lax.rem(x + dx, 4) * 2 + row

        relay = tuple((3 + d, self.along[d]) for d in (2, 1, 3))
        self.todo = [(at(0, 1 - y), 0, relay)]
        for row, base in ((y, 0), (1 - y, 3)):
            self.todo += [(at(4 - d, row), base + d, ()) for d in (1, 3, 2)]

    def start(self, owner, n, device):
        here = self.piece(owner)
        copy = remote(here, here, self.send.at[n], self.recv.at[n], device)
        copy.start()
        self.copies.append(copy)

    def push(self):
        self.start(self.tp, 0, self.beside)
        for d in (2, 1, 3):
            self.start(self.tp, d, self.along[d])

    def collect(self, count=NTP):
        while self.todo and count:
            owner, n, onward = self.todo.pop(0)
            here = self.piece(owner)
            remote(here, here, self.send.at[n], self.recv.at[n], self.beside).wait_recv()
            for later, device in onward:
                self.start(owner, later, device)
            count -= 1
            if self.passed is None:
                continue
            part = self.passed(owner)
            copy = remote(part, part, self.f_send.at[n], self.f_recv.at[n], sibling())
            copy.start()
            self.copies.append(copy)
            self.taken.append((owner, n))

    def settle(self):
        owner, n = self.taken.pop(0)
        part = self.given(owner)
        remote(part, part, self.f_send.at[n], self.f_recv.at[n], sibling()).wait_recv()
        return owner

    def finish(self):
        self.collect()
        for owner, n in self.taken:
            part = self.given(owner)
            remote(part, part, self.f_send.at[n], self.f_recv.at[n], sibling()).wait_recv()

    def drain(self):
        for copy in self.copies:
            copy.wait_send()


class Exchange(Share):
    def __init__(self, piece, passed, given, sems, source=None):
        super().__init__(piece, passed, given, sems)
        self.source = source or (lambda i: piece(self.tp))
        self.todo = [(lax.rem(self.tp - i + NTP, NTP), i, ()) for i in range(1, NTP)]

    def push(self):
        for i in range(1, NTP):
            copy = remote(
                self.source(i), self.piece(self.tp), self.send.at[i], self.recv.at[i], tp_at(i)
            )
            copy.start()
            self.copies.append(copy)


def gelu_pair(pre, tan_pre):
    c = math.sqrt(2.0 / math.pi)
    square = pre * pre
    t = jnp.tanh(c * (pre + 0.044715 * (square * pre)))
    half = 0.5 * (1.0 + t)
    slope = half + 0.5 * pre * (1.0 - t * t) * (c * (1.0 + 3.0 * 0.044715 * square))
    return pre * half, slope * tan_pre


def columns_to_rows(columns):
    lane = lax.broadcasted_iota(jnp.int32, (BLK, BLK), 1)
    packed = jnp.zeros((BLK, BLK), F32)
    for n, column in enumerate(columns):
        packed = jnp.where(lane == n, column, packed)
    return packed.T[0:8]


def rows_to_columns(rows):
    return jnp.concatenate([rows, jnp.zeros((BLK - 8, BLK), F32)], axis=0).T


def body(
    lat, probes, mod, gains, pattern, wqkv_hbm, wout_hbm, wup_hbm, wdn_hbm,
    lat_out, dens_out,
    kv_0, kv_1, kv_2, kv_3,
    wqkv, wo, wmlp, x, xa_0, xa_1, sg, signs, proj, queries, hid, acc, part, got, cross, tot, stat, dens,
    w_sem, s_send, s_recv, r_send, r_recv, p_send, p_recv, d_send, d_recv,
    *many_sems,
):
    ring_sems, share_sems = many_sems[:4], many_sems[4:]
    ctx, tp, core = place()
    column, y = lax.div(tp, 2), lax.rem(tp, 2)
    mine = feature_cols(tp)
    rows_sent = pl.ds(pl.multiple_of(core * HALF, HALF), 3 * HALF)
    my_half = pl.ds(pl.multiple_of(core * (W // 2), HALF), W // 2)
    other_half = pl.ds(pl.multiple_of((1 - core) * (W // 2), HALF), W // 2)
    full = float(D)
    shard = pl.ds(pl.multiple_of(ctx * SHARD, 64), SHARD)
    loads = [
        pltpu.make_async_copy(wup_hbm, wmlp.at[0, shard], w_sem.at[0]),
        pltpu.make_async_copy(wdn_hbm, wmlp.at[1, shard], w_sem.at[1]),
        pltpu.make_async_copy(wqkv_hbm.at[1, :, 0:256], wqkv.at[:, 0:256], w_sem.at[2]),
        pltpu.make_async_copy(wqkv_hbm.at[2, :, 0:256], wqkv.at[:, 256:512], w_sem.at[3]),
        pltpu.make_async_copy(wqkv_hbm.at[1, :, 256:W], wqkv.at[:, 512:640], w_sem.at[6]),
        pltpu.make_async_copy(wqkv_hbm.at[2, :, 256:W], wqkv.at[:, 640:768], w_sem.at[7]),
        pltpu.make_async_copy(wqkv_hbm.at[0], wqkv.at[:, 2 * W : 3 * W], w_sem.at[4]),
        pltpu.make_async_copy(wout_hbm.at[:, mine], wo.at[tp], w_sem.at[5]),
    ]
    for load in loads:
        load.start()
    signs[...] = 2.0 * probes[...].astype(F32) - 1.0
    lat_out[...] = lat[...]
    right, left, across = ring_devices()
    greet([tp_at(i) for i in range(1, NTP)] + [right, left, across, sibling()])

    def block_rows(block, part):
        start = block * SHARD + part * (SHARD - HALF)
        return pl.ds(pl.multiple_of(start, HALF), HALF if part else SHARD - HALF)

    weight_ring = Ring(
        lambda block, part: wmlp.at[core, block_rows(block, part)],
        lambda block, part: wmlp.at[core, block_rows(block, part)],
        lambda block, part: wmlp.at[1 - core, block_rows(block, part)],
        [sems.at[STEPS * NG] for sems in ring_sems],
    )
    wout_share = Exchange(
        lambda owner: wo.at[owner, my_half],
        lambda owner: wo.at[owner, my_half],
        lambda owner: wo.at[owner, other_half],
        [sems.at[STEPS * (NG + 1)] for sems in share_sems],
        lambda i: wout_hbm.at[my_half, feature_cols(lax.rem(tp + i, NTP))],
    )
    sg[:, mine] = signs[...].astype(BF16)
    sign_share = Exchange(
        lambda owner: sg.at[:, feature_cols(owner)],
        None,
        None,
        [sems.at[STEPS * (NG + 1) + 1] for sems in share_sems],
    )
    sign_share.push()
    loads[0].wait()
    loads[1].wait()
    weight_ring.start()
    change = jnp.zeros((BLK, 1), F32)

    for step in range(STEPS):
        copies = []
        kvs = (kv_0, kv_1, kv_2, kv_3)[NG * step : NG * (step + 1)]
        xas = (xa_0, xa_1)
        rows, tangent = lat_out[...], signs[...]
        stat[tp] = columns_to_rows(
            [
                jnp.sum(rows, 1, keepdims=True),
                jnp.sum(rows * rows, 1, keepdims=True),
                jnp.sum(tangent, 1, keepdims=True),
                jnp.sum(rows * tangent, 1, keepdims=True),
            ]
        )
        for i in range(1, NTP):
            copy = remote(
                stat.at[tp], stat.at[tp], s_send.at[step, i], s_recv.at[step, i], tp_at(i)
            )
            copy.start()
            copies.append(copy)
        for i in range(1, NTP):
            there = stat.at[lax.rem(tp - i + NTP, NTP)]
            remote(there, there, s_send.at[step, i], s_recv.at[step, i], tp_at(i)).wait_recv()
        total = stat[0]
        for n in range(1, NTP):
            total = total + stat[n]
        total = rows_to_columns(total) * (1.0 / full)
        row_mean, row_sq, tan_mean, tan_sq = (total[:, n : n + 1] for n in range(4))
        row_var = row_sq - row_mean * row_mean
        tan_var = 2.0 * (tan_sq - row_mean * tan_mean)
        inv_std = lax.rsqrt(row_var + EPS)
        centred = rows - row_mean
        shift, gain = mod[3 * step : 3 * step + 1, mine], 1.0 + mod[3 * step + 1 : 3 * step + 2, mine]
        normed = (centred * inv_std * gain + shift).astype(BF16)
        x[0:HALF, mine] = normed[0:HALF]
        x[3 * HALF : ROWS, mine] = normed[HALF:BLK]
        x_share = Exchange(
            lambda owner: x.at[half_rows(core), feature_cols(owner)],
            lambda owner: x.at[half_rows(core), feature_cols(owner)],
            lambda owner: x.at[half_rows(1 - core), feature_cols(owner)],
            [sems.at[step] for sems in share_sems],
        )
        x_share.push()
        if step == 0:
            weight_ring.advance(2)
            sign_share.finish()
            weight_ring.advance(2)
        inv_rows = jnp.broadcast_to(inv_std, (BLK, W))
        mean_rows = jnp.broadcast_to(inv_std * tan_mean, (BLK, W))
        var_rows = jnp.broadcast_to(0.5 * inv_std * inv_std * tan_var, (BLK, W))

        def rebuild(cols):
            primal = jnp.concatenate([x[0:HALF, cols], x[3 * HALF : ROWS, cols]], axis=0)
            scaled = primal.astype(F32) - mod[3 * step : 3 * step + 1, cols]
            turned = (inv_rows * sg[:, cols].astype(F32) - mean_rows) * (
                1.0 + mod[3 * step + 1 : 3 * step + 2, cols]
            )
            x[HALF : 3 * HALF, cols] = (turned - var_rows * scaled).astype(BF16)

        rebuild(mine)
        for i in range(1, NTP):
            x_share.collect(1)
            if step == 0 and i == 4:
                weight_ring.advance(2)
            if i > 1:
                rebuild(feature_cols(x_share.settle()))
        rebuild(feature_cols(x_share.settle()))
        if step == 0:
            for load in loads[2:]:
                load.wait()

        def head_pair(column, gain_row, h):
            view = proj[:, column : column + HD]
            primal = jnp.concatenate([view[0:HALF], view[3 * HALF : ROWS]], axis=0)
            tan = view[HALF : 3 * HALF]
            gain_view = gains[gain_row : gain_row + 1, h * HD : (h + 1) * HD]
            inv = lax.rsqrt(jnp.mean(primal * primal, 1, keepdims=True) + EPS)
            tan_inv = -inv * inv * inv * jnp.mean(primal * tan, 1, keepdims=True)
            return (
                (primal * inv * gain_view).astype(BF16),
                ((tan * inv + primal * tan_inv) * gain_view).astype(BF16),
            )

        def project(start, stop):
            proj[:, start:stop] = jnp.dot(
                x[...], wqkv[:, start:stop], preferred_element_type=F32
            )

        def own_block(g):
            kv = kvs[g]
            for n, h in enumerate(GROUPS[g]):
                key_at, value_at = (h * HD, 256 + h * HD) if g == 0 else (512, 640)
                key, tan_key = head_pair(key_at, 1, h)
                cols, to = slice(value_at, value_at + HD), slice(n * HD, (n + 1) * HD)
                kv[ctx, 0, :, to] = key
                kv[ctx, 1, :, to] = tan_key
                kv[ctx, 2, :, to] = proj[HALF : 3 * HALF, cols].astype(BF16)
                kv[ctx, 3, 0:HALF, to] = proj[0:HALF, cols].astype(BF16)
                kv[ctx, 3, HALF:BLK, to] = proj[3 * HALF : ROWS, cols].astype(BF16)

        def part_rows(part):
            return slice(part * HALF, (part + 1) * HALF)

        rings = [
            Ring(
                lambda block, part, kv=kv: kv.at[block, pl.ds(core, 3), part_rows(part)],
                lambda block, part, kv=kv: kv.at[block, pl.ds(core * 3, 1), part_rows(part)],
                lambda block, part, kv=kv: kv.at[block, pl.ds((1 - core) * 3, 1), part_rows(part)],
                [sems.at[step * NG + g] for sems in ring_sems],
            )
            for g, kv in enumerate(kvs)
        ]
        shares = [
            (Share, Exchange)[g](
                lambda owner, xa=xa, g=g: xa.at[rows_sent, group_cols(owner, len(GROUPS[g]))],
                lambda owner, xa=xa, g=g: xa.at[half_rows(core), group_cols(owner, len(GROUPS[g]))],
                lambda owner, xa=xa, g=g: xa.at[
                    half_rows(1 - core), group_cols(owner, len(GROUPS[g]))
                ],
                [sems.at[STEPS + step * NG + g] for sems in share_sems],
            )
            for g, xa in enumerate(xas)
        ]
        project(0, 256)
        project(256, 512)
        own_block(0)
        rings[0].start()
        if step == 0:
            weight_ring.advance(4)
            wout_share.push()
        project(512, 768)
        own_block(1)
        project(768, 1152)
        for h in range(HEADS):
            query, tan_query = head_pair(768 + h * HD, 0, h)
            queries[0:BLK, h * HD : (h + 1) * HD] = query
            queries[BLK:ROWS, h * HD : (h + 1) * HD] = tan_query
        if step == 0:
            while weight_ring.todo:
                weight_ring.advance(2)
                rings[0].advance(1)
            weight_ring.finish()

        def up(n):
            cols = slice(256 * n, 256 * (n + 1))
            pre = jnp.dot(x[...], wmlp[0, :, cols], preferred_element_type=F32)
            primal = jnp.concatenate([pre[0:HALF], pre[3 * HALF : ROWS]], axis=0)
            hidden, tan_hidden = gelu_pair(primal, pre[HALF : 3 * HALF])
            hidden = hidden.astype(BF16)
            hid[0:HALF, cols] = hidden[0:HALF]
            hid[HALF : 3 * HALF, cols] = tan_hidden.astype(BF16)
            hid[3 * HALF : ROWS, cols] = hidden[HALF:BLK]

        def down(d, k):
            row = y if k == 0 else 1 - y
            units = feature_cols(lax.rem(column + d, 4) * 2 + row)
            part[d, k] = lax.dot_general(
                hid[...], wmlp[1, units, :], (((1,), (1,)), ((), ())), preferred_element_type=F32
            ).astype(BF16)
            if d and k:
                copy = remote(
                    part.at[d, :, rows_sent],
                    got.at[d - 1],
                    r_send.at[step, d],
                    r_recv.at[step, d],
                    tp_of(column + d, y),
                )
                copy.start()
                copies.append(copy)

        def collect_column():
            for d in range(1, 4):
                remote(
                    got.at[d - 1], got.at[d - 1], r_send.at[step, d], r_recv.at[step, d], sibling()
                ).wait_recv()
            total = part[0, 1, rows_sent].astype(F32)
            for d in range(3):
                total = total + got[d, 1].astype(F32)
            cross[0] = total.astype(BF16)
            copy = remote(
                cross.at[0],
                cross.at[1],
                r_send.at[step, 0],
                r_recv.at[step, 0],
                tp_of(column, 1 - y),
            )
            copy.start()
            copies.append(copy)

        def collect_parts():
            total = part[0, 0, rows_sent].astype(F32)
            for d in range(3):
                total = total + got[d, 0].astype(F32)
            remote(
                cross.at[1], cross.at[1], r_send.at[step, 0], r_recv.at[step, 0], sibling()
            ).wait_recv()
            tot[rows_sent] = total + cross[1].astype(F32)
            piece = tot.at[half_rows(core)]
            copy = remote(piece, piece, p_send.at[step], p_recv.at[step], sibling())
            copy.start()
            copies.append(copy)

        first = pattern[0, 0]
        listed = [pattern[0, j] for j in range(K_SEL)]
        penalty = [
            jnp.where(listed[j] == first, NEG_BIG, 0.0).astype(F32) if j else None
            for j in range(K_SEL)
        ]
        scale = 1.0 / math.sqrt(HD)
        contract = (((1,), (1,)), ((), ()))

        def attend(g, n):
            kv, xa, h = kvs[g], xas[g], GROUPS[g][n]
            own = slice(n * HD, (n + 1) * HD)
            pair = queries[:, h * HD : (h + 1) * HD]
            scores, tan_scores = [], []
            for j in range(K_SEL):
                key, tan_key = kv[listed[j], 0, :, own], kv[listed[j], 1, :, own]
                both = lax.dot_general(pair, key, contract, preferred_element_type=F32) * scale
                crossed = lax.dot_general(
                    pair[0:BLK], tan_key, contract, preferred_element_type=F32
                )
                score = both[0:BLK]
                scores.append(score + penalty[j] if j else score)
                tan_scores.append(both[BLK:ROWS] + crossed * scale)
            top = scores[0]
            for j in range(1, K_SEL):
                top = jnp.maximum(top, scores[j])
            top = jnp.max(top, 1, keepdims=True)
            out = jnp.zeros((ROWS, 2 * HD), F32)
            weight_sum, tan_sum = jnp.zeros((BLK, BLK), F32), jnp.zeros((BLK, BLK), F32)
            for j in range(K_SEL):
                weights = jnp.exp(scores[j] - top)
                weighted = weights * tan_scores[j]
                weight_sum, tan_sum = weight_sum + weights, tan_sum + weighted
                left_side = jnp.concatenate([weights, weighted], axis=0).astype(BF16)
                values = jnp.concatenate(
                    [kv[listed[j], 3, :, own], kv[listed[j], 2, :, own]], axis=1
                )
                out = out + jnp.dot(left_side, values, preferred_element_type=F32)
            inv = 1.0 / jnp.sum(weight_sum, 1, keepdims=True)
            ratio = jnp.sum(tan_sum, 1, keepdims=True) * inv
            output = out[0:BLK, 0:HD] * inv
            tan_output = (out[0:BLK, HD : 2 * HD] + out[BLK:ROWS, 0:HD]) * inv - ratio * output
            output = output.astype(BF16)
            cols = pl.ds(pl.multiple_of((tp * len(GROUPS[g]) + n) * HD, 128), HD)
            xa[0:HALF, cols] = output[0:HALF]
            xa[HALF : 3 * HALF, cols] = tan_output.astype(BF16)
            xa[3 * HALF : ROWS, cols] = output[HALF:BLK]

        def out_project(g):
            size = len(GROUPS[g]) * HD
            rows = wo[:, GROUPS[g][0] * HD : GROUPS[g][0] * HD + size].reshape(NTP * size, W)
            more = jnp.dot(xas[g][...], rows, preferred_element_type=F32)
            acc[...] = more if g == 0 else acc[...] + more

        tasks = [partial(up, n) for n in range(3)] + [
            partial(down, d, k) for d in (2, 1, 3, 0) for k in (0, 1)
        ]
        had = 30 - len(rings[0].todo)
        agenda = [(k, 1, rings[0].advance) for k in range(had, 30)]
        agenda += [(max(9, had), 0, rings[1].start)]
        agenda += [(15 + k, 2, rings[1].advance) for k in range(30)]
        agenda += [(had + 1 + n * (1.6 if step else 1.1), 3, task) for n, task in enumerate(tasks)]
        agenda += [
            (30, 4, rings[0].finish),
            (30, 5, partial(attend, 0, 0)),
            (33, 5, partial(attend, 0, 1)),
            (33, 6, shares[0].push),
            (36, 5, collect_column),
            (38, 5, partial(shares[0].collect, 1)),
            (45, 5, rings[1].finish),
            (45, 6, partial(attend, 1, 0)),
            (45, 7, shares[1].push),
            (46, 0, shares[0].finish),
            (46, 1, collect_parts),
        ]
        if step == 0:
            agenda += [(40, 5, wout_share.collect), (46, 2, wout_share.finish)]
        for _, _, task in sorted(agenda, key=lambda entry: entry[:2]):
            task()
        out_project(0)
        other = tot.at[half_rows(1 - core)]
        remote(other, other, p_send.at[step], p_recv.at[step], sibling()).wait_recv()
        shares[1].finish()
        out_project(1)
        branch = acc[...] + tot[...]
        gate = mod[3 * step + 2 : 3 * step + 3, mine]
        change = change + jnp.sum(
            signs[...] * (gate * branch[HALF : 3 * HALF]), axis=1, keepdims=True
        )
        lat_out[0:HALF] += (1.0 / STEPS) * (gate * branch[0:HALF])
        lat_out[HALF:BLK] += (1.0 / STEPS) * (gate * branch[3 * HALF : ROWS])
        for copy in copies:
            copy.wait_send()
        for part_of in rings + shares + [x_share] + ([weight_ring, wout_share, sign_share] if step == 0 else []):
            part_of.drain()

    copies = []
    dens[tp] = columns_to_rows([change])
    for i in range(1, NTP):
        copy = remote(dens.at[tp], dens.at[tp], d_send.at[i], d_recv.at[i], tp_at(i))
        copy.start()
        copies.append(copy)
    for i in range(1, NTP):
        there = dens.at[lax.rem(tp - i + NTP, NTP)]
        remote(there, there, d_send.at[i], d_recv.at[i], tp_at(i)).wait_recv()
    total = dens[0]
    for n in range(1, NTP):
        total = total + dens[n]
    dens[NTP] = total
    copy = remote(dens.at[NTP], dens.at[NTP + 1], d_send.at[0], d_recv.at[0], sibling())
    copy.start()
    remote(dens.at[NTP + 1], dens.at[NTP + 1], d_send.at[0], d_recv.at[0], sibling()).wait_recv()
    copies.append(copy)
    dens_out[...] = (dens[NTP] + dens[NTP + 1]) * (-1.0 / (STEPS * 2 * math.sqrt(full)))
    for copy in copies:
        copy.wait_send()


def local(latent, probes, modulation, pattern, w_qkv, w_out, w_up, w_down, q_gain, k_gain):
    mod = modulation.reshape(3 * STEPS, D)
    gains = jnp.stack([q_gain, k_gain])
    vmem, anywhere = pl.BlockSpec(memory_space=pltpu.VMEM), pl.BlockSpec(memory_space=pl.ANY)
    dma = pltpu.SemaphoreType.DMA
    latent_out, density = pl.pallas_call(
        body,
        out_shape=(
            jax.ShapeDtypeStruct((BLK, W), F32),
            jax.ShapeDtypeStruct((8, BLK), F32),
        ),
        in_specs=[vmem] * 4 + [pl.BlockSpec(memory_space=pltpu.SMEM)] + [anywhere] * 4,
        out_specs=(vmem, vmem),
        scratch_shapes=[
            pltpu.VMEM((NCTX, 4, BLK, len(group) * HD), BF16)
            for _ in range(STEPS)
            for group in GROUPS
        ]
        + [
            pltpu.VMEM((D, 3 * W), BF16),
            pltpu.VMEM((NTP, W, W), BF16),
            pltpu.VMEM((2, D, UNITS), BF16),
            pltpu.VMEM((ROWS, D), BF16),
            pltpu.VMEM((ROWS, NTP * len(GROUPS[0]) * HD), BF16),
            pltpu.VMEM((ROWS, NTP * len(GROUPS[1]) * HD), BF16),
            pltpu.VMEM((BLK, D), BF16),
            pltpu.VMEM((BLK, W), F32),
            pltpu.VMEM((ROWS, 3 * W), F32),
            pltpu.VMEM((ROWS, W), BF16),
            pltpu.VMEM((ROWS, UNITS), BF16),
            pltpu.VMEM((ROWS, W), F32),
            pltpu.VMEM((4, 2, ROWS, W), BF16),
            pltpu.VMEM((3, 2, 3 * HALF, W), BF16),
            pltpu.VMEM((2, 3 * HALF, W), BF16),
            pltpu.VMEM((ROWS, W), F32),
            pltpu.VMEM((NTP, 8, BLK), F32),
            pltpu.VMEM((NTP + 2, 8, BLK), F32),
            dma((8,)),
        ]
        + [dma((STEPS, NTP)) for _ in range(4)]
        + [dma((STEPS,)) for _ in range(2)]
        + [dma((NTP,)) for _ in range(2)]
        + [dma((STEPS * NG + 1, 30)) for _ in range(4)]
        + [dma((STEPS * (NG + 1) + 2, NTP)) for _ in range(4)],
        compiler_params=pltpu.CompilerParams(
            collective_id=1, has_side_effects=True, vmem_limit_bytes=60 * 1024 * 1024
        ),
        name="euler_steps",
    )(
        latent,
        probes[0],
        mod,
        gains,
        pattern,
        w_qkv.transpose(1, 0, 2),
        w_out,
        w_up,
        w_down.T,
    )
    return latent_out, density[0]


def solution(mesh):
    return jax.shard_map(
        local,
        mesh=mesh,
        in_specs=(
            P("ctx", "tp"),
            P("probe", "ctx", "tp"),
            P(),
            P("ctx", None),
            P(None, None, "tp"),
            P("tp", None),
            P("ctx", "tp"),
            P("tp", "ctx"),
            P("tp"),
            P("tp"),
        ),
        out_specs=(P("ctx", "tp"), P("ctx")),
        check_vma=False,
    )
```
